256 devices in a mesh: date: 64 (over z_hi, x, y), az: 4 (over z_lo, core).
Axes of the slice: x: 4, y: 4, z: 8 (z_hi: 4, z_lo: 2; z = z_hi * 2 + z_lo), core: 2. Of those that a mesh axis runs over, the one named last changes fastest.
Arguments:
- slc: bfloat16 [128, 2, 256, 3072], P('date', None, 'az'), may hold values from -12 to 12
- az_shift: int32 [128], P('date'), may hold values from -4 to 4, as said below
- rg_shift: int32 [128], P('date'), may hold values from -4 to 4, as said below
- az_frac: int32 [128], P('date'), may hold values from 0 to 15
- rg_frac: int32 [128], P('date'), may hold values from 0 to 15
Outputs:
- coherence: bfloat16 [192, 64, 2, 128], P('date', 'az')
- mean_coherence: float32 [192, 64], P('date', 'az')
The draws below stay inside these ranges and needn't reach their ends.
Inputs may be any that keep to these rules, and one draw needn't show every extreme that they name: `az_shift`: date 0 has offset 0; some date has offset 4 and some -4. `rg_shift`: date 0 has offset 0; some date has offset 4 and some -4.
All inputs are finite; a program needn't handle non-finite values.
Results may differ from the reference program's by a relative error of at most 0.0035.
Values may be sent and summed in bfloat16 or wider, within the bound.
No kernel may reach another device: no remote copies, remote signals or barrier semaphores. Data moves between devices by JAX's collectives and lax.ppermute only.
A program may use at most 64 MiB of HBM per device.

```python
import math
import jax
import jax.numpy as jnp
from jax import lax

COLS = 3072
TAPS = 8
KBANK = 16
MAXOFF = 4
LOOK_AZ = 4
LOOK_RG = 16
WINDOW = 7
DATES = 128
ROWS = 256


def shift_table(key, which_axis):
    base_key = jax.random.fold_in(key, 7001 + which_axis)
    drawn = jax.random.randint(base_key, (DATES,), -MAXOFF, MAXOFF + 1, dtype=jnp.int32)
    ordering = jax.random.permutation(jax.random.fold_in(base_key, 3), DATES - 1) + 1
    drawn = drawn.at[0].set(0)
    drawn = drawn.at[ordering[0]].set(MAXOFF)
    drawn = drawn.at[ordering[1]].set(-MAXOFF)
    return drawn.astype(jnp.int32)


def draw_az_shift(key, part):
    return shift_table(key, 0)


def draw_rg_shift(key, part):
    return shift_table(key, 1)


def draw_slc(key, part):
    az_table = shift_table(key, 0)
    rg_table = shift_table(key, 1)
    scene_key = jax.random.fold_in(key, 9001)
    extent = (2, ROWS + 2 * MAXOFF, COLS + 2 * MAXOFF)
    scene = jax.random.truncated_normal(jax.random.fold_in(scene_key, 1), -4.0, 4.0, extent, jnp.float32)
    strength = jax.random.uniform(jax.random.fold_in(scene_key, 2), (DATES,), jnp.float32, 0.3, 1.0).at[0].set(1.0)
    phases = jax.random.uniform(jax.random.fold_in(scene_key, 3), (DATES,), jnp.float32, -math.pi, math.pi).at[0].set(0.0)
    noise_key = jax.random.fold_in(scene_key, 4)

    def one_date(date_pos):
        shifted = lax.dynamic_slice(scene, (jnp.int32(0), (MAXOFF - az_table[date_pos]).astype(jnp.int32), (MAXOFF - rg_table[date_pos]).astype(jnp.int32)), (2, ROWS, COLS))
        cosine = jnp.cos(phases[date_pos])
        sine = jnp.sin(phases[date_pos])
        rotated = jnp.stack([shifted[0] * cosine - shifted[1] * sine, shifted[0] * sine + shifted[1] * cosine])
        noise = jax.random.truncated_normal(jax.random.fold_in(noise_key, date_pos), -4.0, 4.0, (2, ROWS, COLS), jnp.float32)
        weight = strength[date_pos]
        mixed = weight * rotated + jnp.sqrt(1.0 - weight * weight) * noise
        return mixed.astype(jnp.bfloat16)
    return lax.map(one_date, jnp.arange(DATES, dtype=jnp.int32))


def place_ends(values, own_key, least, top_value):
    shape = values.shape
    place = [jax.random.randint(jax.random.fold_in(own_key, axis), (), 0, shape[axis]) for axis in range(len(shape))]
    values = values.at[tuple(place)].set(least)
    longest = shape.index(max(shape))
    place[longest] = (place[longest] + 1) % shape[longest]
    return values.at[tuple(place)].set(top_value)


def setup_inputs(seed: int = 0) -> dict:
    seeds = jax.random.split(jax.random.key(seed), 6)
    return {
        "slc": draw_slc(jax.random.fold_in(seeds[5], 71), 0),
        "az_shift": draw_az_shift(jax.random.fold_in(seeds[5], 71), 0),
        "rg_shift": draw_rg_shift(jax.random.fold_in(seeds[5], 71), 0),
        "az_frac": place_ends(jax.random.randint(seeds[3], (DATES,), 0, KBANK), jax.random.fold_in(seeds[3], 1), 0, KBANK - 1).astype(jnp.int32),
        "rg_frac": place_ends(jax.random.randint(seeds[4], (DATES,), 0, KBANK), jax.random.fold_in(seeds[4], 1), 0, KBANK - 1).astype(jnp.int32),
    }


EPS = 1e-06

def kernel_bank():
    fraction = jnp.arange(KBANK, dtype=jnp.float32)[:, None] / KBANK
    tap_place = jnp.arange(TAPS, dtype=jnp.float32)[None, :]
    offset = tap_place - (TAPS // 2 - 1) - fraction
    shaped = jnp.sinc(offset) * (0.5 + 0.5 * jnp.cos(jnp.pi * offset / (TAPS // 2 + 0.5)))
    return shaped / lax.optimization_barrier(jnp.sum(shaped, axis=1, keepdims=True))

def looks_of(values):
    lead = values.shape[:-2]
    rows_in, cols_in = (values.shape[-2], values.shape[-1])
    boxed = values.reshape(lead + (rows_in // LOOK_AZ, LOOK_AZ, cols_in // LOOK_RG, LOOK_RG))
    return lax.optimization_barrier(jnp.mean(boxed, axis=(-3, -1)))

def window_sum(padded):
    radius = WINDOW // 2
    rows_out = padded.shape[-2] - 2 * radius
    cols_out = padded.shape[-1] - 2 * radius
    across = padded[..., 0:rows_out, :]
    for offset_row in range(1, WINDOW):
        across = across + padded[..., offset_row:offset_row + rows_out, :]
    total = across[..., 0:cols_out]
    for offset_col in range(1, WINDOW):
        total = total + across[..., offset_col:offset_col + cols_out]
    return total

def reference(slc, az_shift, rg_shift, az_frac, rg_frac):
    bank = kernel_bank()
    margin = MAXOFF + TAPS // 2
    center = slc[0].astype(jnp.float32)
    power_ref = looks_of(center[0] * center[0] + center[1] * center[1])

    def one_date(packed):
        image, az_offset, rg_offset, az_weights, rg_weights = packed
        padded = jnp.pad(image, ((0, 0), (margin, margin), (margin, margin)))
        ranged = jnp.zeros((2, ROWS + 2 * margin, COLS), jnp.float32)
        for tap_place in range(TAPS):
            start = (margin + rg_offset + tap_place - (TAPS // 2 - 1)).astype(jnp.int32)
            ranged = ranged + rg_weights[tap_place] * lax.dynamic_slice_in_dim(padded, start, COLS, 2).astype(jnp.float32)
        resampled = jnp.zeros((2, ROWS, COLS), jnp.float32)
        for tap_place in range(TAPS):
            start = (margin + az_offset + tap_place - (TAPS // 2 - 1)).astype(jnp.int32)
            resampled = resampled + az_weights[tap_place] * lax.dynamic_slice_in_dim(ranged, start, ROWS, 1)
        real_part = center[0] * resampled[0] + center[1] * resampled[1]
        imag_part = center[1] * resampled[0] - center[0] * resampled[1]
        power_sec = resampled[0] * resampled[0] + resampled[1] * resampled[1]
        return looks_of(jnp.stack([real_part, imag_part, power_sec]))
    looks = lax.map(one_date, (slc, az_shift, rg_shift, bank[az_frac], bank[rg_frac]))
    radius = WINDOW // 2
    summed = window_sum(jnp.pad(looks, ((0, 0), (0, 0), (radius, radius), (radius, radius))))
    summed_ref = window_sum(jnp.pad(power_ref, ((radius, radius), (radius, radius))))
    scale = 1.0 / jnp.sqrt(summed_ref[None] * summed[:, 2] + EPS)
    gamma = jnp.stack([summed[:, 0] * scale, summed[:, 1] * scale], axis=1).astype(jnp.bfloat16)
    gamma = lax.optimization_barrier(gamma)
    as_float = gamma.astype(jnp.float32)
    magnitude = jnp.sqrt(as_float[:, 0] * as_float[:, 0] + as_float[:, 1] * as_float[:, 1])
    average = lax.optimization_barrier(jnp.mean(magnitude, axis=0))
    return (jnp.transpose(gamma, (3, 2, 1, 0)), jnp.transpose(average, (1, 0)))
```

```python
import functools

import jax
import jax.numpy as jnp
import numpy as np
from jax import lax
from jax.experimental import pallas as pl
from jax.experimental.pallas import tpu as pltpu
from jax.sharding import PartitionSpec as P

TAPS = 8
KBANK = 16
LOOK_AZ = 4
LOOK_RG = 16
RADIUS = 3
EPS = 1e-06
ROWS = 64
COLS = 3072
TILE = 256
NT = COLS // TILE
LOOKS = ROWS // LOOK_AZ
LCOLS = COLS // LOOK_RG
F32 = jnp.float32
BF16 = jnp.bfloat16
VMEM = pltpu.MemorySpace.VMEM
SMEM = pltpu.MemorySpace.SMEM


def kernel_bank():
    fraction = np.arange(KBANK)[:, None] / KBANK
    offset = np.arange(TAPS)[None, :] - (TAPS // 2 - 1) - fraction
    shaped = np.sinc(offset) * (0.5 + 0.5 * np.cos(np.pi * offset / (TAPS // 2 + 0.5)))
    return (shaped / shaped.sum(axis=1, keepdims=True)).astype(np.float32)


def iota(shape, dim):
    return lax.broadcasted_iota(jnp.int32, shape, dim)


def two_halves(value):
    high = value.astype(BF16)
    return high, (value - high.astype(F32)).astype(BF16)


def dot(a, b, dims=((1,), (0,))):
    return lax.dot_general(a, b, (dims, ((), ())), preferred_element_type=F32)


def band(tap_of, weight):
    total = jnp.zeros(tap_of.shape, F32)
    for tap in range(TAPS):
        total = jnp.where(tap_of == tap, weight(tap), total)
    return two_halves(total)


def resample_kernel(
    date, azs, rgs, azf, rgf, bank, own, before, after, out, rows_in, wide_hi, wide_lo
):
    source = iota((ROWS, ROWS + 16), 1)
    source = jnp.where(
        source < ROWS, source, jnp.where(source < ROWS + 8, source - ROWS - 8, source - 8)
    )
    az_frac = azf[date]
    rg_frac = rgf[date]
    az_hi, az_lo = band(
        source - iota((ROWS, ROWS + 16), 0) - azs[date] + (TAPS // 2 - 1),
        lambda tap: bank[az_frac, tap],
    )
    az_both = jnp.concatenate([az_hi, az_lo], axis=0)
    half = TILE // 2
    rg_hi, rg_lo = band(
        iota((2 * TILE, TILE), 0) - half - iota((2 * TILE, TILE), 1) - rgs[date] + (TAPS // 2 - 1),
        lambda tap: bank[rg_frac, tap],
    )
    blank = jnp.zeros((ROWS, half), BF16)
    for part in range(2):
        rows_in[0:ROWS] = own[0, part]
        rows_in[ROWS : ROWS + 16] = jnp.concatenate(
            [before[0, part].astype(F32), after[0, part].astype(F32)], axis=0
        ).astype(BF16)
        for tile in range(NT + 1):
            first = max(tile * TILE - half, 0)
            last = min(tile * TILE + half, COLS)
            both = dot(az_both, rows_in[:, first:last])
            pieces = two_halves(both[:ROWS] + both[ROWS:])
            for piece, wide in zip(pieces, (wide_hi, wide_lo)):
                if tile == 0:
                    piece = jnp.concatenate([blank, piece], axis=1)
                if tile == NT:
                    piece = jnp.concatenate([piece, blank], axis=1)
                place = part * ROWS
                if tile < NT:
                    at = tile * 2 * ROWS + place
                    wide[at : at + ROWS, 0:TILE] = piece
                if tile > 0:
                    at = (tile - 1) * 2 * ROWS + place
                    wide[at : at + ROWS, TILE : 2 * TILE] = piece
    out[...] = dot(wide_hi[...], rg_hi) + (dot(wide_lo[...], rg_hi) + dot(wide_hi[...], rg_lo))


def resample(date, scalars, slc, before, after):
    return pl.pallas_call(
        functools.partial(resample_kernel, date),
        name=f"resample{date}",
        grid=(1,),
        out_shape=jax.ShapeDtypeStruct((NT * 2 * ROWS, TILE), F32),
        in_specs=[pl.BlockSpec(memory_space=SMEM)] * 5
        + [
            pl.BlockSpec((1, 2, ROWS, COLS), lambda i: (date, 0, 0, 0)),
            pl.BlockSpec((1, 2, 8, COLS), lambda i: (date, 0, 0, 0)),
            pl.BlockSpec((1, 2, 8, COLS), lambda i: (date, 0, 0, 0)),
        ],
        out_specs=pl.BlockSpec((NT * 2 * ROWS, TILE), lambda i: (0, 0)),
        scratch_shapes=[
            pltpu.VMEM((ROWS + 16, COLS), BF16),
            pltpu.VMEM((NT * 2 * ROWS, 2 * TILE), BF16),
            pltpu.VMEM((NT * 2 * ROWS, 2 * TILE), BF16),
        ],
        cost_estimate=pl.CostEstimate(
            flops=3_000_000_000, transcendentals=0, bytes_accessed=2_600_000
        ),
    )(*scalars, slc, before, after)


def looks_kernel(center, first, second, out, columns):
    columns[...] = jnp.zeros(columns.shape, F32)
    reach = iota((32, TILE), 1) // LOOK_RG + 8 - iota((32, TILE), 0)
    box = jnp.where(jnp.abs(reach) <= RADIUS, 1.0, 0.0).astype(BF16)
    for tile in range(NT):
        at = tile * TILE
        e0 = center[0:8, :, at : at + TILE].astype(F32).reshape(ROWS, TILE)
        e1 = center[8:16, :, at : at + TILE].astype(F32).reshape(ROWS, TILE)
        cross = []
        power = []
        for stack in (first, second):
            s0 = stack[tile * 2 * ROWS : tile * 2 * ROWS + ROWS]
            s1 = stack[tile * 2 * ROWS + ROWS : (tile + 1) * 2 * ROWS]
            cross.append(e0 * s0 + e1 * s1)
            cross.append(e1 * s0 - e0 * s1)
            power.append(s0 * s0 + s1 * s1)
        power.append(e0 * e0 + e1 * e1)
        high, low = two_halves(jnp.concatenate(cross + power, axis=0))
        nt = ((1,), (1,))
        columns[tile * 16 : tile * 16 + 32] += dot(box, high, nt) + dot(box, low, nt)
    quantities = 7
    pixel = iota((quantities * ROWS, 128), 0)
    box_rows = jnp.where(pixel // LOOK_AZ == iota((quantities * ROWS, 128), 1), 1.0 / 64, 0.0)
    box_rows = box_rows.astype(BF16)
    high, low = two_halves(columns[8 : 8 + LCOLS])
    out[...] = dot(high, box_rows) + dot(low, box_rows)


def looks(center, first, second):
    return pl.pallas_call(
        looks_kernel,
        name="looks",
        out_shape=jax.ShapeDtypeStruct((LCOLS, 128), F32),
        in_specs=[pl.BlockSpec(memory_space=VMEM)] * 3,
        out_specs=pl.BlockSpec(memory_space=VMEM),
        scratch_shapes=[pltpu.VMEM((LCOLS + 16, 7 * ROWS), F32)],
    )(center, first, second)


def coherence_kernel(own, before, after, out, kept):
    source = iota((384, 384), 0)
    target = iota((384, 384), 1)
    row_in = source % 16 + (source // 128) * 16 - 16
    lane = source % 128
    quantity = lane // 16
    group = target // 128
    slot = target % 128
    date = slot // 32
    wanted = jnp.where(
        group == 0, date * 2 + slot % 2, jnp.where(group == 1, 4 + date, 6)
    )
    reach = row_in - (slot % 32) // 2
    hit = (quantity == wanted) & (jnp.abs(reach) <= RADIUS) & (slot < 64)
    box = jnp.where(hit, 1.0, 0.0).astype(BF16)
    high, low = two_halves(jnp.concatenate([before[...], own[...], after[...]], axis=1))
    summed = dot(high, box) + dot(low, box)
    cross = summed[:, 0:128]
    scale = 1.0 / jnp.sqrt(summed[:, 256:384] * summed[:, 128:256] + EPS)
    kept[...] = cross * scale
    third = LCOLS // 3
    pieces = [kept[pl.ds(k, third, stride=3), :] for k in range(3)]
    out[:, 0:128] = jnp.concatenate([pieces[0][:, 0:64], pieces[1][:, 0:64]], axis=1).astype(BF16)
    out[:, 128:256] = pieces[2].astype(BF16)


def coherence(own, before, after):
    return pl.pallas_call(
        coherence_kernel,
        name="coherence",
        out_shape=jax.ShapeDtypeStruct((LCOLS // 3, 256), BF16),
        in_specs=[pl.BlockSpec(memory_space=VMEM)] * 3,
        out_specs=pl.BlockSpec(memory_space=VMEM),
        scratch_shapes=[pltpu.VMEM((LCOLS, 128), F32)],
    )(own, before, after)


def finish_kernel(arrived, out, mean):
    source = iota((64, 128), 0)
    lane = iota((64, 128), 1)
    tn = ((0,), (0,))
    packed = arrived[:, 0:192]
    placed = []
    for date in range(2):
        spread = jnp.where(lane == source * 2 + date, 1.0, 0.0).astype(BF16)
        placed.append(dot(packed, spread, tn))
    rows = jnp.concatenate(
        [placed[0][k * 64 : k * 64 + 32] + placed[1][k * 64 + 32 : k * 64 + 64] for k in range(3)],
        axis=0,
    )
    out[...] = rows.astype(BF16)
    square = rows * rows
    pair = jnp.where(iota((48, 96), 1) // 2 == iota((48, 96), 0), 1.0, 0.0)
    exact = lax.Precision.HIGHEST
    magnitude = jnp.sqrt(jnp.dot(pair, square, precision=exact, preferred_element_type=F32))
    share = jnp.full((8, 128), 1.0 / 128, F32)
    mean[...] = lax.dot_general(
        share, magnitude, (((1,), (1,)), ((), ())), precision=exact, preferred_element_type=F32
    )


def finish(arrived):
    return pl.pallas_call(
        finish_kernel,
        name="finish",
        out_shape=(jax.ShapeDtypeStruct((96, 128), BF16), jax.ShapeDtypeStruct((8, 48), F32)),
        in_specs=[pl.BlockSpec(memory_space=VMEM)],
        out_specs=(pl.BlockSpec(memory_space=VMEM), pl.BlockSpec(memory_space=VMEM)),
    )(arrived)


def place(z, x, y):
    return z * 16 + x * 4 + y


def broadcast_center(center):
    four = range(4)
    first = lax.axis_index("date") == 0
    quarter = jnp.where(first, center[0:4], jnp.zeros_like(center[0:4]))
    for k in range(1, 4):
        pairs = [(place(0, 0, 0), place(0, k, 0))]
        quarter = quarter + lax.ppermute(center[4 * k : 4 * k + 4], "date", pairs)
    chunk = quarter[0:1]
    for k in range(1, 4):
        pairs = [(place(0, x, 0), place(0, x, k)) for x in four]
        chunk = chunk + lax.ppermute(quarter[k : k + 1], "date", pairs)
    whole = chunk
    for k in range(1, 4):
        pairs = [(place(0, x, y), place(k, x, y)) for x in four for y in four]
        whole = whole + lax.ppermute(chunk, "date", pairs)
    planes = [[place(z, x, y) for x in four for y in four] for z in four]
    copies = jnp.broadcast_to(whole, (16,) + whole.shape[1:])
    return lax.all_to_all(copies, "date", 0, 0, axis_index_groups=planes, tiled=True)


def body(slc, az_shift, rg_shift, az_frac, rg_frac):
    up = [(i, i + 1) for i in range(3)]
    down = [(i + 1, i) for i in range(3)]
    center = broadcast_center(slc[0].reshape(16, 8, COLS))
    before = lax.ppermute(slc[:, :, ROWS - 8 :], "az", up)
    after = lax.ppermute(slc[:, :, :8], "az", down)
    scalars = (az_shift, rg_shift, az_frac, rg_frac, jnp.asarray(kernel_bank()))
    stacks = [resample(date, scalars, slc, before, after) for date in range(2)]
    own = looks(center, *stacks)
    outgoing = coherence(own, lax.ppermute(own, "az", up), lax.ppermute(own, "az", down))
    arrived = lax.all_to_all(
        outgoing.reshape(64, 2, 128), "date", split_axis=0, concat_axis=0, tiled=True
    )
    rows, mean = finish(arrived.reshape(64, 256))
    return rows.reshape(3, LOOKS, 2, 128), mean[0].reshape(3, LOOKS)


def solution(mesh):
    placed = (P("date", None, "az", None), P("date"), P("date"), P("date"), P("date"))
    return jax.shard_map(
        body,
        mesh=mesh,
        in_specs=placed,
        out_specs=(P("date", "az", None, None), P("date", "az")),
        check_vma=False,
    )
```

```python
import functools

import jax
import jax.numpy as jnp
import numpy as np
from jax import lax
from jax.experimental import pallas as pl
from jax.experimental.pallas import tpu as pltpu
from jax.sharding import PartitionSpec as P


TAPS = 8
KBANK = 16
LOOK_AZ = 4
LOOK_RG = 16
RADIUS = 3
EPS = 1e-06
ROWS = 64
COLS = 3072
TILE = 256
NT = COLS // TILE
LOOKS = ROWS // LOOK_AZ
LCOLS = COLS // LOOK_RG
F32 = jnp.float32
BF16 = jnp.bfloat16
VMEM = pltpu.VMEM
SMEM = pltpu.SMEM

GRANT = pltpu.CompilerParams(vmem_limit_bytes=20 * 2**20)


def kernel_bank():
    fraction = np.arange(KBANK)[:, None] / KBANK
    offset = np.arange(TAPS)[None, :] - (TAPS // 2 - 1) - fraction
    shaped = np.sinc(offset) * (0.5 + 0.5 * np.cos(np.pi * offset / (TAPS // 2 + 0.5)))
    return (shaped / shaped.sum(axis=1, keepdims=True)).astype(np.float32)


def iota(shape, dim):
    return lax.broadcasted_iota(jnp.int32, shape, dim)


def near(*arrays):
    return [pltpu.with_memory_space_constraint(a, VMEM) for a in arrays]


def two_halves(value):
    high = value.astype(BF16)
    return high, (value - high.astype(F32)).astype(BF16)


def dot(a, b, dims=((1,), (0,))):
    return lax.dot_general(a, b, (dims, ((), ())), preferred_element_type=F32)


def band(tap_of, weight):
    total = jnp.zeros(tap_of.shape, F32)
    for tap in range(TAPS):
        total = jnp.where(tap_of == tap, weight(tap), total)
    return two_halves(total)


def resample_kernel(
    date, azs, rgs, azf, rgf, bank, own, before, after, out, rows_in, wide_hi, wide_lo, arrived
):
    copies = [
        pltpu.make_async_copy(own.at[date, part], rows_in.at[part, 0:ROWS], arrived.at[part])
        for part in range(2)
    ]
    for copy in copies:
        copy.start()
    source = iota((ROWS, ROWS + 16), 1)
    source = jnp.where(
        source < ROWS, source, jnp.where(source < ROWS + 8, source - ROWS - 8, source - 8)
    )
    az_frac = azf[date]
    rg_frac = rgf[date]
    az_hi, az_lo = band(
        source - iota((ROWS, ROWS + 16), 0) - azs[date] + (TAPS // 2 - 1),
        lambda tap: bank[az_frac, tap],
    )
    az_both = jnp.concatenate([az_hi, az_lo], axis=0)
    half = TILE // 2
    rg_hi, rg_lo = band(
        iota((2 * TILE, TILE), 0) - half - iota((2 * TILE, TILE), 1) - rgs[date] + (TAPS // 2 - 1),
        lambda tap: bank[rg_frac, tap],
    )
    blank = jnp.zeros((ROWS, half), BF16)
    for part in range(2):
        rows_in[part, ROWS : ROWS + 16] = jnp.concatenate(
            [before[date, part].astype(F32), after[date, part].astype(F32)], axis=0
        ).astype(BF16)
        copies[part].wait()
        for tile in range(NT + 1):
            first = max(tile * TILE - half, 0)
            last = min(tile * TILE + half, COLS)
            both = dot(az_both, rows_in[part, :, first:last])
            pieces = two_halves(both[:ROWS] + both[ROWS:])
            for piece, wide in zip(pieces, (wide_hi, wide_lo)):
                if tile == 0:
                    piece = jnp.concatenate([blank, piece], axis=1)
                if tile == NT:
                    piece = jnp.concatenate([piece, blank], axis=1)
                place = part * ROWS
                if tile < NT:
                    at = tile * 2 * ROWS + place
                    wide[at : at + ROWS, 0:TILE] = piece
                if tile > 0:
                    at = (tile - 1) * 2 * ROWS + place
                    wide[at : at + ROWS, TILE : 2 * TILE] = piece
    out[...] = dot(wide_hi[...], rg_hi) + (dot(wide_lo[...], rg_hi) + dot(wide_hi[...], rg_lo))


def resample(date, scalars, slc, before, after):
    return pl.pallas_call(
        functools.partial(resample_kernel, date),
        compiler_params=GRANT,
        out_shape=VMEM((NT * 2 * ROWS, TILE), F32),
        in_specs=[pl.BlockSpec(memory_space=SMEM)] * 5
        + [pl.BlockSpec(memory_space=pl.ANY)]
        + [pl.BlockSpec(memory_space=VMEM)] * 2,
        out_specs=pl.BlockSpec(memory_space=VMEM),
        scratch_shapes=[
            pltpu.VMEM((2, ROWS + 16, COLS), BF16),
            pltpu.VMEM((NT * 2 * ROWS, 2 * TILE), BF16),
            pltpu.VMEM((NT * 2 * ROWS, 2 * TILE), BF16),
            pltpu.SemaphoreType.DMA((2,)),
        ],
        cost_estimate=pl.CostEstimate(
            flops=3_000_000_000, transcendentals=0, bytes_accessed=1_600_000
        ),
    )(*scalars, slc, *near(before, after))


def looks_kernel(center, first, second, out, columns):
    columns[...] = jnp.zeros(columns.shape, F32)
    reach = iota((32, TILE), 1) // LOOK_RG + 8 - iota((32, TILE), 0)
    box = jnp.where(jnp.abs(reach) <= RADIUS, 1.0, 0.0).astype(BF16)
    for tile in range(NT):
        at = tile * TILE
        e0 = center[0:8, :, at : at + TILE].astype(F32).reshape(ROWS, TILE)
        e1 = center[8:16, :, at : at + TILE].astype(F32).reshape(ROWS, TILE)
        cross = []
        power = []
        for stack in (first, second):
            s0 = stack[tile * 2 * ROWS : tile * 2 * ROWS + ROWS]
            s1 = stack[tile * 2 * ROWS + ROWS : (tile + 1) * 2 * ROWS]
            cross.append(e0 * s0 + e1 * s1)
            cross.append(e1 * s0 - e0 * s1)
            power.append(s0 * s0 + s1 * s1)
        power.append(e0 * e0 + e1 * e1)
        high, low = two_halves(jnp.concatenate(cross + power, axis=0))
        nt = ((1,), (1,))
        columns[tile * 16 : tile * 16 + 32] += dot(box, high, nt) + dot(box, low, nt)
    quantities = 7
    pixel = iota((quantities * ROWS, 128), 0)
    box_rows = jnp.where(pixel // LOOK_AZ == iota((quantities * ROWS, 128), 1), 1.0 / 64, 0.0)
    box_rows = box_rows.astype(BF16)
    high, low = two_halves(columns[8 : 8 + LCOLS])
    out[...] = dot(high, box_rows) + dot(low, box_rows)


def looks(center, first, second):
    return pl.pallas_call(
        looks_kernel,
        name="looks",
        compiler_params=GRANT,
        out_shape=VMEM((LCOLS, 128), F32),
        in_specs=[pl.BlockSpec(memory_space=VMEM)] * 3,
        out_specs=pl.BlockSpec(memory_space=VMEM),
        scratch_shapes=[pltpu.VMEM((LCOLS + 16, 7 * ROWS), F32)],
    )(*near(center, first, second))


def coherence_kernel(own, before, after, out, kept):
    source = iota((384, 384), 0)
    target = iota((384, 384), 1)
    row_in = source % 16 + (source // 128) * 16 - 16
    lane = source % 128
    quantity = lane // 16
    group = target // 128
    slot = target % 128
    date = slot // 32
    wanted = jnp.where(
        group == 0, date * 2 + slot % 2, jnp.where(group == 1, 4 + date, 6)
    )
    reach = row_in - (slot % 32) // 2
    hit = (quantity == wanted) & (jnp.abs(reach) <= RADIUS) & (slot < 64)
    box = jnp.where(hit, 1.0, 0.0).astype(BF16)
    high, low = two_halves(jnp.concatenate([before[...], own[...], after[...]], axis=1))
    summed = dot(high, box) + dot(low, box)
    cross = summed[:, 0:128]
    scale = 1.0 / jnp.sqrt(summed[:, 256:384] * summed[:, 128:256] + EPS)
    kept[...] = cross * scale
    third = LCOLS // 3
    pieces = [kept[pl.ds(k, third, stride=3), :] for k in range(3)]
    pair = jnp.concatenate([pieces[0][:, 0:64], pieces[1][:, 0:64]], axis=1)
    out[...] = jnp.stack([pair, pieces[2]], axis=1).astype(BF16)


def coherence(own, before, after):
    return pl.pallas_call(
        coherence_kernel,
        name="coherence",
        compiler_params=GRANT,
        out_shape=VMEM((LCOLS // 3, 2, 128), BF16),
        in_specs=[pl.BlockSpec(memory_space=VMEM)] * 3,
        out_specs=pl.BlockSpec(memory_space=VMEM),
        scratch_shapes=[pltpu.VMEM((LCOLS, 128), F32)],
    )(*near(own, before, after))


def finish_kernel(arrived, out, mean):
    source = iota((64, 128), 0)
    lane = iota((64, 128), 1)
    tn = ((0,), (0,))
    wide = arrived[...].astype(F32)
    packed = jnp.concatenate([wide[:, 0], wide[:, 1, 0:64]], axis=1).astype(BF16)
    placed = []
    for date in range(2):
        spread = jnp.where(lane == source * 2 + date, 1.0, 0.0).astype(BF16)
        placed.append(dot(packed, spread, tn))
    rows = jnp.concatenate(
        [placed[0][k * 64 : k * 64 + 32] + placed[1][k * 64 + 32 : k * 64 + 64] for k in range(3)],
        axis=0,
    )
    out[...] = rows.astype(BF16)
    square = rows * rows
    pair = jnp.where(iota((48, 96), 1) // 2 == iota((48, 96), 0), 1.0, 0.0)
    exact = lax.Precision.HIGHEST
    magnitude = jnp.sqrt(jnp.dot(pair, square, precision=exact, preferred_element_type=F32))
    share = jnp.full((8, 128), 1.0 / 128, F32)
    average = lax.dot_general(
        share, magnitude, (((1,), (1,)), ((), ())), precision=exact, preferred_element_type=F32
    )
    for k in range(3):
        mean[k : k + 1] = average[0:1, k * LOOKS : (k + 1) * LOOKS]


def finish(arrived):
    return pl.pallas_call(
        finish_kernel,
        name="finish",
        compiler_params=GRANT,
        out_shape=(
            jax.ShapeDtypeStruct((96, 128), BF16),
            jax.ShapeDtypeStruct((3, LOOKS), F32),
        ),
        in_specs=[pl.BlockSpec(memory_space=VMEM)],
        out_specs=(pl.BlockSpec(memory_space=VMEM), pl.BlockSpec(memory_space=VMEM)),
    )(*near(arrived))


def place(z, x, y):
    return z * 16 + x * 4 + y


HOMES = (
    ((0, 0), (0, 3), (1, 3), (3, 3)),
    ((1, 0), (2, 0), (1, 1), (2, 1)),
    ((3, 0), (3, 1), (3, 2), (2, 3)),
    ((0, 1), (0, 2), (1, 2), (2, 2)),
)


def body(slc, az_shift, rg_shift, az_frac, rg_frac):
    up = [(i, i + 1) for i in range(3)]
    down = [(i + 1, i) for i in range(3)]
    scalars = (az_shift, rg_shift, az_frac, rg_frac, jnp.asarray(kernel_bank()))
    quarters = [
        slc[0, part, 32 * half : 32 * half + 32].reshape(4, 8, COLS)
        for part in range(2)
        for half in range(2)
    ]

    first = lax.axis_index("date") == 0
    pieces = [lax.ppermute(quarters[k], "date", [(0, place(0, *HOMES[k][0]))]) for k in range(1, 4)]
    before = lax.ppermute(slc[:, :, ROWS - 8 :], "az", up)
    after = lax.ppermute(slc[:, :, :8], "az", down)
    pieces, before, after = lax.optimization_barrier((pieces, before, after))
    quarter = jnp.where(first, quarters[0], jnp.zeros_like(quarters[0])) + sum(pieces)

    pieces = [
        lax.ppermute(
            quarter[k : k + 1],
            "date",
            [(place(0, *homes[0]), place(0, *homes[k])) for homes in HOMES],
        )
        for k in range(1, 4)
    ]
    early = resample(0, scalars, slc, before, after)
    pieces, early = lax.optimization_barrier((pieces, early))
    chunk = quarter[0:1] + sum(pieces)

    flat = [home for homes in HOMES for home in homes]
    pieces = [
        lax.ppermute(chunk, "date", [(place(0, *home), place(k, *home)) for home in flat])
        for k in (2, 1, 3)
    ]
    late = resample(1, scalars, slc, before, after)
    pieces, late = lax.optimization_barrier((pieces, late))
    whole = chunk + sum(pieces)

    planes = [[place(z, *home) for home in flat] for z in range(4)]
    copies = jnp.broadcast_to(whole, (16,) + whole.shape[1:])
    center = lax.all_to_all(copies, "date", 0, 0, axis_index_groups=planes, tiled=True)
    own = looks(center, early, late)
    outgoing = coherence(own, lax.ppermute(own, "az", up), lax.ppermute(own, "az", down))
    arrived = lax.all_to_all(outgoing, "date", split_axis=0, concat_axis=0, tiled=True)
    rows, mean = finish(arrived)
    return rows.reshape(3, LOOKS, 2, 128), mean


def solution(mesh):
    placed = (P("date", None, "az", None), P("date"), P("date"), P("date"), P("date"))
    return jax.shard_map(
        body,
        mesh=mesh,
        in_specs=placed,
        out_specs=(P("date", "az", None, None), P("date", "az")),
        check_vma=False,
    )
```

```python
import functools

import jax
import jax.numpy as jnp
import numpy as np
from jax import lax
from jax.experimental import pallas as pl
from jax.experimental.pallas import tpu as pltpu
from jax.sharding import PartitionSpec as P


TAPS = 8
KBANK = 16
LOOK_AZ = 4
LOOK_RG = 16
RADIUS = 3
EPS = 1e-06
ROWS = 64
COLS = 3072
TILE = 256
NT = COLS // TILE
LOOKS = ROWS // LOOK_AZ
LCOLS = COLS // LOOK_RG
F32 = jnp.float32
BF16 = jnp.bfloat16
VMEM = pltpu.VMEM
SMEM = pltpu.SMEM

GRANT = pltpu.CompilerParams(vmem_limit_bytes=20 * 2**20)


def kernel_bank():
    fraction = np.arange(KBANK)[:, None] / KBANK
    offset = np.arange(TAPS)[None, :] - (TAPS // 2 - 1) - fraction
    shaped = np.sinc(offset) * (0.5 + 0.5 * np.cos(np.pi * offset / (TAPS // 2 + 0.5)))
    return (shaped / shaped.sum(axis=1, keepdims=True)).astype(np.float32)


def iota(shape, dim):
    return lax.broadcasted_iota(jnp.int32, shape, dim)


def near(*arrays):
    return [pltpu.with_memory_space_constraint(a, VMEM) for a in arrays]


def far_away(*arrays):
    return [pltpu.with_memory_space_constraint(a, pltpu.HBM) for a in arrays]


def two_halves(value):
    high = value.astype(BF16)
    return high, (value - high.astype(F32)).astype(BF16)


def dot(a, b, dims=((1,), (0,))):
    return lax.dot_general(a, b, (dims, ((), ())), preferred_element_type=F32)


def band(tap_of, weight):
    total = jnp.zeros(tap_of.shape, F32)
    for tap in range(TAPS):
        total = jnp.where(tap_of == tap, weight(tap), total)
    return two_halves(total)


def odd_block():
    return lax.rem(lax.axis_index("az"), 2) == 1


def in_order(partner, other):
    odd = odd_block()
    return [jnp.where(odd, partner, other), jnp.where(odd, other, partner)]


def swapped(to_partner, to_other):
    return (
        lax.ppermute(to_partner, "az", [(0, 1), (1, 0), (2, 3), (3, 2)]),
        lax.ppermute(to_other, "az", [(1, 2), (2, 1)]),
    )


def resample_kernel(
    date,
    azs,
    rgs,
    azf,
    rgf,
    bank,
    own,
    partner,
    other,
    near_out,
    *rest,
):
    *far_out, power, rows_in, edges, wide_hi, wide_lo, arrived = rest
    copies = [
        pltpu.make_async_copy(source.at[date], edges.at[at], arrived.at[2 + at])
        for at, source in enumerate((partner, other))
    ] + [
        pltpu.make_async_copy(own.at[date, part], rows_in.at[part, 0:ROWS], arrived.at[part])
        for part in range(2)
    ]
    for copy in copies:
        copy.start()
    source = iota((ROWS, ROWS + 16), 1)
    source = jnp.where(
        source < ROWS, source, jnp.where(source < ROWS + 8, source - ROWS - 8, source - 8)
    )
    az_frac = azf[date]
    rg_frac = rgf[date]
    az_hi, az_lo = band(
        source - iota((ROWS, ROWS + 16), 0) - azs[date] + (TAPS // 2 - 1),
        lambda tap: bank[az_frac, tap],
    )
    az_both = jnp.concatenate([az_hi, az_lo], axis=0)
    half = TILE // 2
    rg_hi, rg_lo = band(
        iota((2 * TILE, TILE), 0) - half - iota((2 * TILE, TILE), 1) - rgs[date] + (TAPS // 2 - 1),
        lambda tap: bank[rg_frac, tap],
    )
    blank = jnp.zeros((ROWS, half), BF16)
    for part in range(2):
        if part == 0:
            copies[0].wait()
            copies[1].wait()
        pair = edges[0, part].astype(F32), edges[1, part].astype(F32)
        rows_in[part, ROWS : ROWS + 16] = jnp.concatenate(
            in_order(*pair), axis=0
        ).astype(BF16)
        copies[2 + part].wait()
        for tile in range(NT + 1):
            first = max(tile * TILE - half, 0)
            last = min(tile * TILE + half, COLS)
            both = dot(az_both, rows_in[part, :, first:last])
            pieces = two_halves(both[:ROWS] + both[ROWS:])
            for piece, wide in zip(pieces, (wide_hi, wide_lo)):
                if tile == 0:
                    piece = jnp.concatenate([blank, piece], axis=1)
                if tile == NT:
                    piece = jnp.concatenate([piece, blank], axis=1)
                place = part * ROWS
                if tile < NT:
                    at = tile * 2 * ROWS + place
                    wide[at : at + ROWS, 0:TILE] = piece
                if tile > 0:
                    at = (tile - 1) * 2 * ROWS + place
                    wide[at : at + ROWS, TILE : 2 * TILE] = piece
    at = 0
    stacks = [near_out] + far_out
    for stack in stacks:
        count = stack.shape[0]
        hi, lo = wide_hi[at : at + count], wide_lo[at : at + count]
        stack[...] = dot(hi, rg_hi) + (dot(lo, rg_hi) + dot(hi, rg_lo))
        at += count
    power[...] = jnp.zeros(power.shape, F32)
    box = column_box()
    for tile in range(NT):
        s0, s1 = both_parts(stacks, tile)
        add_columns(power, box, tile, s0 * s0 + s1 * s1)


def column_box():
    reach = iota((32, TILE), 1) // LOOK_RG + 8 - iota((32, TILE), 0)
    return jnp.where(jnp.abs(reach) <= RADIUS, 1.0, 0.0).astype(BF16)


def both_parts(stacks, tile):
    at = tile * 2 * ROWS
    for stack in stacks:
        if at < stack.shape[0]:
            break
        at -= stack.shape[0]
    return stack[at : at + ROWS], stack[at + ROWS : at + 2 * ROWS]


def add_columns(columns, box, tile, values):
    high, low = two_halves(values)
    nt = ((1,), (1,))
    columns[tile * 16 : tile * 16 + 32] += dot(box, high, nt) + dot(box, low, nt)


def resample(date, far, scalars, slc, partner, other):
    spaces = (VMEM, pltpu.HBM) if far else (VMEM,)
    rows = NT * 2 * ROWS // len(spaces)
    return pl.pallas_call(
        functools.partial(resample_kernel, date),
        compiler_params=GRANT,
        out_shape=tuple(space((rows, TILE), F32) for space in spaces)
        + (VMEM((LCOLS + 16, ROWS), F32),),
        in_specs=[pl.BlockSpec(memory_space=SMEM)] * 5
        + [pl.BlockSpec(memory_space=pl.ANY)] * 3,
        out_specs=(pl.BlockSpec(memory_space=VMEM),) * (len(spaces) + 1),
        scratch_shapes=[
            pltpu.VMEM((2, ROWS + 16, COLS), BF16),
            pltpu.VMEM((2, 2, 8, COLS), BF16),
            pltpu.VMEM((NT * 2 * ROWS, 2 * TILE), BF16),
            pltpu.VMEM((NT * 2 * ROWS, 2 * TILE), BF16),
            pltpu.SemaphoreType.DMA((4,)),
        ],
        cost_estimate=pl.CostEstimate(
            flops=3_000_000_000, transcendentals=0, bytes_accessed=1_600_000
        ),
    )(*scalars, *far_away(slc, partner, other))


FAR = NT * ROWS


def looks_kernel(center, near_first, second, power0, power1, far, out, columns, far_first, arrived):
    copy = pltpu.make_async_copy(far, far_first, arrived)
    copy.start()
    box = column_box()
    columns[...] = jnp.zeros(columns.shape, F32)
    for tile in range(NT):
        if tile == NT // 2:
            copy.wait()
        at = tile * TILE
        e0 = center[0:8, :, at : at + TILE].astype(F32).reshape(ROWS, TILE)
        e1 = center[8:16, :, at : at + TILE].astype(F32).reshape(ROWS, TILE)
        values = []
        for stacks in ((near_first, far_first), (second,)):
            s0, s1 = both_parts(stacks, tile)
            values += [e0 * s0 + e1 * s1, e1 * s0 - e0 * s1]
        values.append(e0 * e0 + e1 * e1)
        add_columns(columns, box, tile, jnp.concatenate(values, axis=0))

    total = jnp.zeros((LCOLS, 128), F32)
    quantity = 0
    for part in (columns, power0, power1):
        shape = (part.shape[1], 128)
        hit = iota(shape, 0) // LOOK_AZ == iota(shape, 1) - quantity * LOOKS
        box_rows = jnp.where(hit, 1.0 / (LOOK_AZ * LOOK_RG), 0.0).astype(BF16)
        high, low = two_halves(part[8 : 8 + LCOLS])
        total = total + (dot(high, box_rows) + dot(low, box_rows))
        quantity += part.shape[1] // ROWS
    out[...] = total


def looks(center, near_first, far_first, second, power0, power1):
    return pl.pallas_call(
        looks_kernel,
        name="looks",
        compiler_params=GRANT,
        out_shape=VMEM((LCOLS, 128), F32),
        in_specs=[pl.BlockSpec(memory_space=VMEM)] * 5 + [pl.BlockSpec(memory_space=pl.ANY)],
        out_specs=pl.BlockSpec(memory_space=VMEM),
        scratch_shapes=[
            pltpu.VMEM((LCOLS + 16, 5 * ROWS), F32),
            pltpu.VMEM((FAR, TILE), F32),
            pltpu.SemaphoreType.DMA,
        ],
    )(
        *near(center, near_first, second, power0, power1), *far_away(far_first)
    )


def coherence_kernel(own, partner, other, out, kept):
    source = iota((384, 384), 0)
    target = iota((384, 384), 1)
    row_in = source % 16 + (source // 128) * 16 - 16
    lane = source % 128
    quantity = lane // 16
    group = target // 128
    slot = target % 128
    date = slot // 32
    wanted = jnp.where(
        group == 0, date * 2 + slot % 2, jnp.where(group == 1, 5 + date, 4)
    )
    reach = row_in - (slot % 32) // 2
    hit = (quantity == wanted) & (jnp.abs(reach) <= RADIUS) & (slot < 64)
    box = jnp.where(hit, 1.0, 0.0).astype(BF16)
    before, after = in_order(partner[...], other[...])
    high, low = two_halves(jnp.concatenate([before, own[...], after], axis=1))
    summed = dot(high, box) + dot(low, box)
    cross = summed[:, 0:128]
    scale = 1.0 / jnp.sqrt(summed[:, 256:384] * summed[:, 128:256] + EPS)
    kept[...] = cross * scale
    third = LCOLS // 3
    pieces = [kept[pl.ds(k, third, stride=3), :] for k in range(3)]
    pair = jnp.concatenate([pieces[0][:, 0:64], pieces[1][:, 0:64]], axis=1)
    out[...] = jnp.stack([pair, pieces[2]], axis=1).astype(BF16)


def coherence(own, partner, other):
    return pl.pallas_call(
        coherence_kernel,
        name="coherence",
        compiler_params=GRANT,
        out_shape=VMEM((LCOLS // 3, 2, 128), BF16),
        in_specs=[pl.BlockSpec(memory_space=VMEM)] * 3,
        out_specs=pl.BlockSpec(memory_space=VMEM),
        scratch_shapes=[pltpu.VMEM((LCOLS, 128), F32)],
    )(*near(own, partner, other))


def finish_kernel(arrived, out, mean):
    source = iota((64, 128), 0)
    lane = iota((64, 128), 1)
    tn = ((0,), (0,))
    wide = arrived[...].astype(F32)
    packed = jnp.concatenate([wide[:, 0], wide[:, 1, 0:64]], axis=1).astype(BF16)
    placed = []
    for date in range(2):
        spread = jnp.where(lane == source * 2 + date, 1.0, 0.0).astype(BF16)
        placed.append(dot(packed, spread, tn))
    rows = jnp.concatenate(
        [placed[0][k * 64 : k * 64 + 32] + placed[1][k * 64 + 32 : k * 64 + 64] for k in range(3)],
        axis=0,
    )
    out[...] = rows.astype(BF16)
    square = rows * rows
    pair = jnp.where(iota((48, 96), 1) // 2 == iota((48, 96), 0), 1.0, 0.0)
    exact = lax.Precision.HIGHEST
    magnitude = jnp.sqrt(jnp.dot(pair, square, precision=exact, preferred_element_type=F32))
    share = jnp.full((8, 128), 1.0 / 128, F32)
    average = lax.dot_general(
        share, magnitude, (((1,), (1,)), ((), ())), precision=exact, preferred_element_type=F32
    )
    for k in range(3):
        mean[k : k + 1] = average[0:1, k * LOOKS : (k + 1) * LOOKS]


def finish(arrived):
    return pl.pallas_call(
        finish_kernel,
        name="finish",
        compiler_params=GRANT,
        out_shape=(
            jax.ShapeDtypeStruct((96, 128), BF16),
            jax.ShapeDtypeStruct((3, LOOKS), F32),
        ),
        in_specs=[pl.BlockSpec(memory_space=VMEM)],
        out_specs=(pl.BlockSpec(memory_space=VMEM), pl.BlockSpec(memory_space=VMEM)),
    )(*near(arrived))


def quarters_kernel(slc, *rest):
    *outs, arrived = rest
    copies = []
    for out, homes in zip(outs, HOMES):
        for at, (x, y) in enumerate(homes):
            part, block = divmod(x * 4 + y, 8)
            source = slc.at[0, part, pl.ds(block * 8, 8)]
            copies.append(pltpu.make_async_copy(source, out.at[at], arrived.at[len(copies)]))
    for copy in copies:
        copy.start()
    for copy in copies:
        copy.wait()


def quarters_of(slc):
    return pl.pallas_call(
        quarters_kernel,
        name="quarters",
        compiler_params=GRANT,
        out_shape=(VMEM((4, 8, COLS), BF16),) * 4,
        in_specs=[pl.BlockSpec(memory_space=pl.ANY)],
        out_specs=(pl.BlockSpec(memory_space=VMEM),) * 4,
        scratch_shapes=[pltpu.SemaphoreType.DMA((16,))],
    )(*far_away(slc))


def copies_kernel(own, *rest):
    *pieces, out, value, sent = rest
    total = own[0]
    for piece in pieces:
        total = total + piece[0]
    value[...] = total
    copies = [pltpu.make_async_copy(value, out.at[at], sent.at[at]) for at in range(16)]
    for copy in copies:
        copy.start()
    for copy in copies:
        copy.wait()


def copies_of(own, pieces):
    return pl.pallas_call(
        copies_kernel,
        name="copies",
        compiler_params=GRANT,
        out_shape=pltpu.HBM((16, 8, COLS), BF16),
        in_specs=[pl.BlockSpec(memory_space=VMEM)] * 4,
        out_specs=pl.BlockSpec(memory_space=pl.ANY),
        scratch_shapes=[pltpu.VMEM((8, COLS), BF16), pltpu.SemaphoreType.DMA((16,))],
    )(*near(own, *pieces))


def place(z, x, y):
    return z * 16 + x * 4 + y


HOMES = (
    ((0, 0), (0, 3), (1, 3), (3, 3)),
    ((1, 0), (2, 0), (1, 1), (2, 1)),
    ((3, 0), (3, 1), (3, 2), (2, 3)),
    ((0, 1), (0, 2), (1, 2), (2, 2)),
)


def body(slc, az_shift, rg_shift, az_frac, rg_frac):
    scalars = (az_shift, rg_shift, az_frac, rg_frac, jnp.asarray(kernel_bank()))
    quarters = quarters_of(slc)
    kept = jnp.where(lax.axis_index("date") == 0, quarters[0], jnp.zeros_like(quarters[0]))
    kept = lax.optimization_barrier(kept)

    pieces = [lax.ppermute(quarters[k], "date", [(0, place(0, *HOMES[k][0]))]) for k in range(1, 4)]
    head, tail = slc[:, :, :8], slc[:, :, ROWS - 8 :]
    odd = odd_block()
    edges = swapped(jnp.where(odd, head, tail), jnp.where(odd, tail, head))
    quarter = kept + sum(pieces)

    pieces = [
        lax.ppermute(
            quarter[k : k + 1],
            "date",
            [(place(0, *homes[0]), place(0, *homes[k])) for homes in HOMES],
        )
        for k in range(1, 4)
    ]
    chunk = quarter[0:1] + sum(pieces)

    flat = [home for homes in HOMES for home in homes]
    pieces = [
        lax.ppermute(chunk, "date", [(place(0, *home), place(k, *home)) for home in flat])
        for k in (1, 3, 2)
    ]

    planes = [[place(z, x, y) for x in range(4) for y in range(4)] for z in range(4)]
    copies = copies_of(chunk, pieces)
    center = lax.all_to_all(copies, "date", 0, 0, axis_index_groups=planes, tiled=True)
    near_first, far_first, power0 = resample(0, True, scalars, slc, *edges)
    second, power1 = resample(1, False, scalars, slc, *edges)
    own = looks(center, near_first, far_first, second, power0, power1)
    outgoing = coherence(own, *swapped(own, own))
    arrived = lax.all_to_all(outgoing, "date", split_axis=0, concat_axis=0, tiled=True)
    rows, mean = finish(arrived)
    return rows.reshape(3, LOOKS, 2, 128), mean


def solution(mesh):
    placed = (P("date", None, "az", None), P("date"), P("date"), P("date"), P("date"))
    return jax.shard_map(
        body,
        mesh=mesh,
        in_specs=placed,
        out_specs=(P("date", "az", None, None), P("date", "az")),
        check_vma=False,
    )
```

```python
import functools

import jax
import jax.numpy as jnp
import numpy as np
from jax import lax
from jax.experimental import pallas as pl
from jax.experimental.pallas import tpu as pltpu
from jax.sharding import PartitionSpec as P


TAPS = 8
KBANK = 16
LOOK_AZ = 4
LOOK_RG = 16
RADIUS = 3
EPS = 1e-06
ROWS = 64
COLS = 3072
TILE = 256
NT = COLS // TILE
LOOKS = ROWS // LOOK_AZ
LCOLS = COLS // LOOK_RG
F32 = jnp.float32
BF16 = jnp.bfloat16
VMEM = pltpu.VMEM
SMEM = pltpu.SMEM

GRANT = pltpu.CompilerParams(vmem_limit_bytes=20 * 2**20)


def kernel_bank():
    fraction = np.arange(KBANK)[:, None] / KBANK
    offset = np.arange(TAPS)[None, :] - (TAPS // 2 - 1) - fraction
    shaped = np.sinc(offset) * (0.5 + 0.5 * np.cos(np.pi * offset / (TAPS // 2 + 0.5)))
    return (shaped / shaped.sum(axis=1, keepdims=True)).astype(np.float32)


def iota(shape, dim):
    return lax.broadcasted_iota(jnp.int32, shape, dim)


def near(*arrays):
    return [pltpu.with_memory_space_constraint(a, VMEM) for a in arrays]


def far_away(*arrays):
    return [pltpu.with_memory_space_constraint(a, pltpu.HBM) for a in arrays]


def two_halves(value):
    high = value.astype(BF16)
    return high, (value - high.astype(F32)).astype(BF16)


def dot(a, b, dims=((1,), (0,))):
    return lax.dot_general(a, b, (dims, ((), ())), preferred_element_type=F32)


def band(tap_of, weight):
    total = jnp.zeros(tap_of.shape, F32)
    for tap in range(TAPS):
        total = jnp.where(tap_of == tap, weight(tap), total)
    return two_halves(total)


def odd_block():
    return lax.rem(lax.axis_index("az"), 2) == 1


def in_order(partner, other):
    odd = odd_block()
    return [jnp.where(odd, partner, other), jnp.where(odd, other, partner)]


def swapped(to_partner, to_other):
    return (
        lax.ppermute(to_partner, "az", [(0, 1), (1, 0), (2, 3), (3, 2)]),
        lax.ppermute(to_other, "az", [(1, 2), (2, 1)]),
    )


def resample_kernel(
    date,
    count,
    *refs,
):
    tables, (own, partner, other), rest = refs[:5], refs[5:8], refs[8:]
    stacks, power = rest[:count], rest[count]
    rows_in, edges, wide_hi, wide_lo, arrived, *local = rest[count + 1 :]
    loads = [
        pltpu.make_async_copy(table, here, arrived.at[4 + at])
        for at, (table, here) in enumerate(zip(tables, local))
    ]
    for load in loads:
        load.start()
    azs, rgs, azf, rgf, bank = local
    copies = [
        pltpu.make_async_copy(source.at[date], edges.at[at], arrived.at[2 + at])
        for at, source in enumerate((partner, other))
    ] + [
        pltpu.make_async_copy(own.at[date, part], rows_in.at[part, 0:ROWS], arrived.at[part])
        for part in range(2)
    ]
    for copy in copies:
        copy.start()
    for load in loads:
        load.wait()
    source = iota((ROWS, ROWS + 16), 1)
    source = jnp.where(
        source < ROWS, source, jnp.where(source < ROWS + 8, source - ROWS - 8, source - 8)
    )
    az_frac = azf[date]
    rg_frac = rgf[date]
    az_hi, az_lo = band(
        source - iota((ROWS, ROWS + 16), 0) - azs[date] + (TAPS // 2 - 1),
        lambda tap: bank[az_frac, tap],
    )
    az_both = jnp.concatenate([az_hi, az_lo], axis=0)
    half = TILE // 2
    rg_hi, rg_lo = band(
        iota((2 * TILE, TILE), 0) - half - iota((2 * TILE, TILE), 1) - rgs[date] + (TAPS // 2 - 1),
        lambda tap: bank[rg_frac, tap],
    )
    blank = jnp.zeros((ROWS, half), BF16)
    for part in range(2):
        if part == 0:
            copies[0].wait()
            copies[1].wait()
        pair = edges[0, part].astype(F32), edges[1, part].astype(F32)
        rows_in[part, ROWS : ROWS + 16] = jnp.concatenate(
            in_order(*pair), axis=0
        ).astype(BF16)
        copies[2 + part].wait()
        for tile in range(NT + 1):
            first = max(tile * TILE - half, 0)
            last = min(tile * TILE + half, COLS)
            both = dot(az_both, rows_in[part, :, first:last])
            pieces = two_halves(both[:ROWS] + both[ROWS:])
            for piece, wide in zip(pieces, (wide_hi, wide_lo)):
                if tile == 0:
                    piece = jnp.concatenate([blank, piece], axis=1)
                if tile == NT:
                    piece = jnp.concatenate([piece, blank], axis=1)
                place = part * ROWS
                if tile < NT:
                    at = tile * 2 * ROWS + place
                    wide[at : at + ROWS, 0:TILE] = piece
                if tile > 0:
                    at = (tile - 1) * 2 * ROWS + place
                    wide[at : at + ROWS, TILE : 2 * TILE] = piece
    at = 0
    for stack in stacks:
        size = stack.shape[0]
        hi, lo = wide_hi[at : at + size], wide_lo[at : at + size]
        stack[...] = dot(hi, rg_hi) + (dot(lo, rg_hi) + dot(hi, rg_lo))
        at += size
    power[...] = jnp.zeros(power.shape, F32)
    box = column_box()
    for tile in range(NT):
        s0, s1 = both_parts(stacks, tile)
        add_columns(power, box, tile, s0 * s0 + s1 * s1)


def column_box():
    reach = iota((32, TILE), 1) // LOOK_RG + 8 - iota((32, TILE), 0)
    return jnp.where(jnp.abs(reach) <= RADIUS, 1.0, 0.0).astype(BF16)


def both_parts(stacks, tile):
    at = tile * 2 * ROWS
    for stack in stacks:
        if at < stack.shape[0]:
            break
        at -= stack.shape[0]
    return stack[at : at + ROWS], stack[at + ROWS : at + 2 * ROWS]


def add_columns(columns, box, tile, values):
    high, low = two_halves(values)
    nt = ((1,), (1,))
    columns[tile * 16 : tile * 16 + 32] += dot(box, high, nt) + dot(box, low, nt)


def resample(date, far, scalars, slc, partner, other):
    spaces = (VMEM, pltpu.HBM) if far else (VMEM,)
    rows = NT * 2 * ROWS // len(spaces)
    return pl.pallas_call(
        functools.partial(resample_kernel, date, len(spaces)),
        compiler_params=GRANT,
        out_shape=tuple(space((rows, TILE), F32) for space in spaces)
        + (VMEM((LCOLS + 16, ROWS), F32),),
        in_specs=[pl.BlockSpec(memory_space=pl.ANY)] * 8,
        out_specs=(pl.BlockSpec(memory_space=VMEM),) * (len(spaces) + 1),
        scratch_shapes=[
            pltpu.VMEM((2, ROWS + 16, COLS), BF16),
            pltpu.VMEM((2, 2, 8, COLS), BF16),
            pltpu.VMEM((NT * 2 * ROWS, 2 * TILE), BF16),
            pltpu.VMEM((NT * 2 * ROWS, 2 * TILE), BF16),
            pltpu.SemaphoreType.DMA((9,)),
        ]
        + [SMEM((2,), jnp.int32)] * 4
        + [SMEM((KBANK, TAPS), F32)],
        cost_estimate=pl.CostEstimate(
            flops=3_000_000_000, transcendentals=0, bytes_accessed=1_600_000
        ),
    )(*far_away(*scalars, slc), partner, other)


FAR = NT * ROWS


def looks_kernel(center, near_first, second, power0, power1, far, out, columns, far_first, arrived):
    copy = pltpu.make_async_copy(far, far_first, arrived)
    copy.start()
    box = column_box()
    columns[...] = jnp.zeros(columns.shape, F32)
    for tile in range(NT):
        if tile == NT // 2:
            copy.wait()
        at = tile * TILE
        e0 = center[0:8, :, at : at + TILE].astype(F32).reshape(ROWS, TILE)
        e1 = center[8:16, :, at : at + TILE].astype(F32).reshape(ROWS, TILE)
        values = []
        for stacks in ((near_first, far_first), (second,)):
            s0, s1 = both_parts(stacks, tile)
            values += [e0 * s0 + e1 * s1, e1 * s0 - e0 * s1]
        values.append(e0 * e0 + e1 * e1)
        add_columns(columns, box, tile, jnp.concatenate(values, axis=0))

    total = jnp.zeros((LCOLS, 128), F32)
    quantity = 0
    for part in (columns, power0, power1):
        shape = (part.shape[1], 128)
        hit = iota(shape, 0) // LOOK_AZ == iota(shape, 1) - quantity * LOOKS
        box_rows = jnp.where(hit, 1.0 / (LOOK_AZ * LOOK_RG), 0.0).astype(BF16)
        high, low = two_halves(part[8 : 8 + LCOLS])
        total = total + (dot(high, box_rows) + dot(low, box_rows))
        quantity += part.shape[1] // ROWS
    out[...] = total


def looks(center, near_first, far_first, second, power0, power1):
    return pl.pallas_call(
        looks_kernel,
        name="looks",
        compiler_params=GRANT,
        out_shape=VMEM((LCOLS, 128), F32),
        in_specs=[pl.BlockSpec(memory_space=VMEM)] * 5 + [pl.BlockSpec(memory_space=pl.ANY)],
        out_specs=pl.BlockSpec(memory_space=VMEM),
        scratch_shapes=[
            pltpu.VMEM((LCOLS + 16, 5 * ROWS), F32),
            pltpu.VMEM((FAR, TILE), F32),
            pltpu.SemaphoreType.DMA,
        ],
    )(
        *near(center, near_first, second, power0, power1), *far_away(far_first)
    )


def coherence_kernel(own, partner, other, out, kept):
    source = iota((384, 384), 0)
    target = iota((384, 384), 1)
    row_in = source % 16 + (source // 128) * 16 - 16
    lane = source % 128
    quantity = lane // 16
    group = target // 128
    slot = target % 128
    date = slot // 32
    wanted = jnp.where(
        group == 0, date * 2 + slot % 2, jnp.where(group == 1, 5 + date, 4)
    )
    reach = row_in - (slot % 32) // 2
    hit = (quantity == wanted) & (jnp.abs(reach) <= RADIUS) & (slot < 64)
    box = jnp.where(hit, 1.0, 0.0).astype(BF16)
    before, after = in_order(partner[...], other[...])
    high, low = two_halves(jnp.concatenate([before, own[...], after], axis=1))
    summed = dot(high, box) + dot(low, box)
    cross = summed[:, 0:128]
    scale = 1.0 / jnp.sqrt(summed[:, 256:384] * summed[:, 128:256] + EPS)
    kept[...] = cross * scale
    third = LCOLS // 3
    pieces = [kept[pl.ds(k, third, stride=3), :] for k in range(3)]
    pair = jnp.concatenate([pieces[0][:, 0:64], pieces[1][:, 0:64]], axis=1)
    out[...] = jnp.stack([pair, pieces[2]], axis=1).astype(BF16)


def coherence(own, partner, other):
    return pl.pallas_call(
        coherence_kernel,
        name="coherence",
        compiler_params=GRANT,
        out_shape=VMEM((LCOLS // 3, 2, 128), BF16),
        in_specs=[pl.BlockSpec(memory_space=VMEM)] * 3,
        out_specs=pl.BlockSpec(memory_space=VMEM),
        scratch_shapes=[pltpu.VMEM((LCOLS, 128), F32)],
    )(*near(own, partner, other))


def finish_kernel(arrived, out, mean):
    source = iota((64, 128), 0)
    lane = iota((64, 128), 1)
    tn = ((0,), (0,))
    wide = arrived[...].astype(F32)
    packed = jnp.concatenate([wide[:, 0], wide[:, 1, 0:64]], axis=1).astype(BF16)
    placed = []
    for date in range(2):
        spread = jnp.where(lane == source * 2 + date, 1.0, 0.0).astype(BF16)
        placed.append(dot(packed, spread, tn))
    rows = jnp.concatenate(
        [placed[0][k * 64 : k * 64 + 32] + placed[1][k * 64 + 32 : k * 64 + 64] for k in range(3)],
        axis=0,
    )
    out[...] = rows.astype(BF16)
    square = rows * rows
    pair = jnp.where(iota((48, 96), 1) // 2 == iota((48, 96), 0), 1.0, 0.0)
    exact = lax.Precision.HIGHEST
    magnitude = jnp.sqrt(jnp.dot(pair, square, precision=exact, preferred_element_type=F32))
    share = jnp.full((8, 128), 1.0 / 128, F32)
    average = lax.dot_general(
        share, magnitude, (((1,), (1,)), ((), ())), precision=exact, preferred_element_type=F32
    )
    for k in range(3):
        mean[k : k + 1] = average[0:1, k * LOOKS : (k + 1) * LOOKS]


def finish(arrived):
    return pl.pallas_call(
        finish_kernel,
        name="finish",
        compiler_params=GRANT,
        out_shape=(
            jax.ShapeDtypeStruct((96, 128), BF16),
            jax.ShapeDtypeStruct((3, LOOKS), F32),
        ),
        in_specs=[pl.BlockSpec(memory_space=VMEM)],
        out_specs=(pl.BlockSpec(memory_space=VMEM), pl.BlockSpec(memory_space=VMEM)),
    )(*near(arrived))


def quarters_kernel(slc, *rest):
    *outs, arrived = rest
    copies = []
    for out, homes in zip(outs, HOMES):
        for at, (x, y) in enumerate(homes):
            part, block = divmod(x * 4 + y, 8)
            source = slc.at[0, part, pl.ds(block * 8, 8)]
            copies.append(pltpu.make_async_copy(source, out.at[at], arrived.at[len(copies)]))
    for copy in copies:
        copy.start()
    for copy in copies:
        copy.wait()


def quarters_of(slc):
    return pl.pallas_call(
        quarters_kernel,
        name="quarters",
        compiler_params=GRANT,
        out_shape=(VMEM((4, 8, COLS), BF16),) * 4,
        in_specs=[pl.BlockSpec(memory_space=pl.ANY)],
        out_specs=(pl.BlockSpec(memory_space=VMEM),) * 4,
        scratch_shapes=[pltpu.SemaphoreType.DMA((16,))],
    )(*far_away(slc))


def copies_kernel(own, *rest):
    *pieces, out, value, sent = rest
    total = own[0]
    for piece in pieces:
        total = total + piece[0]
    value[...] = total
    copies = [pltpu.make_async_copy(value, out.at[at], sent.at[at]) for at in range(16)]
    for copy in copies:
        copy.start()
    for copy in copies:
        copy.wait()


def copies_of(own, pieces):
    return pl.pallas_call(
        copies_kernel,
        name="copies",
        compiler_params=GRANT,
        out_shape=pltpu.HBM((16, 8, COLS), BF16),
        in_specs=[pl.BlockSpec(memory_space=VMEM)] * 4,
        out_specs=pl.BlockSpec(memory_space=pl.ANY),
        scratch_shapes=[pltpu.VMEM((8, COLS), BF16), pltpu.SemaphoreType.DMA((16,))],
    )(*near(own, *pieces))


def place(z, x, y):
    return z * 16 + x * 4 + y


HOMES = (
    ((0, 0), (0, 3), (1, 3), (3, 3)),
    ((1, 0), (2, 0), (1, 1), (2, 1)),
    ((3, 0), (3, 1), (3, 2), (2, 3)),
    ((0, 1), (0, 2), (1, 2), (2, 2)),
)


def body(slc, az_shift, rg_shift, az_frac, rg_frac):
    scalars = (az_shift, rg_shift, az_frac, rg_frac, jnp.asarray(kernel_bank()))
    quarters = quarters_of(slc)
    kept = jnp.where(lax.axis_index("date") == 0, quarters[0], jnp.zeros_like(quarters[0]))
    kept = lax.optimization_barrier(kept)

    pieces = [lax.ppermute(quarters[k], "date", [(0, place(0, *HOMES[k][0]))]) for k in range(1, 4)]
    head, tail = slc[:, :, :8], slc[:, :, ROWS - 8 :]
    odd = odd_block()
    edges = swapped(jnp.where(odd, head, tail), jnp.where(odd, tail, head))
    quarter = kept + sum(pieces)

    pieces = [
        lax.ppermute(
            quarter[k : k + 1],
            "date",
            [(place(0, *homes[0]), place(0, *homes[k])) for homes in HOMES],
        )
        for k in range(1, 4)
    ]
    chunk = quarter[0:1] + sum(pieces)

    flat = [home for homes in HOMES for home in homes]
    pieces = [
        lax.ppermute(chunk, "date", [(place(0, *home), place(k, *home)) for home in flat])
        for k in (1, 3, 2)
    ]
    first = resample(0, True, scalars, slc, *edges)
    pieces, first = lax.optimization_barrier((pieces, first))

    planes = [[place(z, x, y) for x in range(4) for y in range(4)] for z in range(4)]
    copies = copies_of(chunk, pieces)
    center = lax.all_to_all(copies, "date", 0, 0, axis_index_groups=planes, tiled=True)
    near_first, far_first, power0 = first
    second, power1 = resample(1, False, scalars, slc, *edges)
    own = looks(center, near_first, far_first, second, power0, power1)
    outgoing = coherence(own, *swapped(own, own))
    arrived = lax.all_to_all(outgoing, "date", split_axis=0, concat_axis=0, tiled=True)
    rows, mean = finish(arrived)
    return rows.reshape(3, LOOKS, 2, 128), mean


def solution(mesh):
    placed = (P("date", None, "az", None), P("date"), P("date"), P("date"), P("date"))
    return jax.shard_map(
        body,
        mesh=mesh,
        in_specs=placed,
        out_specs=(P("date", "az", None, None), P("date", "az")),
        check_vma=False,
    )
```

```python
import functools

import jax
import jax.numpy as jnp
import numpy as np
from jax import lax
from jax.experimental import pallas as pl
from jax.experimental.pallas import tpu as pltpu
from jax.sharding import PartitionSpec as P


TAPS = 8
KBANK = 16
LOOK_AZ = 4
LOOK_RG = 16
RADIUS = 3
EPS = 1e-06
ROWS = 64
COLS = 3072
TILE = 256
NT = COLS // TILE
LOOKS = ROWS // LOOK_AZ
LCOLS = COLS // LOOK_RG
F32 = jnp.float32
BF16 = jnp.bfloat16
VMEM = pltpu.VMEM
SMEM = pltpu.SMEM

GRANT = pltpu.CompilerParams(vmem_limit_bytes=20 * 2**20)


def kernel_bank():
    fraction = np.arange(KBANK)[:, None] / KBANK
    offset = np.arange(TAPS)[None, :] - (TAPS // 2 - 1) - fraction
    shaped = np.sinc(offset) * (0.5 + 0.5 * np.cos(np.pi * offset / (TAPS // 2 + 0.5)))
    return (shaped / shaped.sum(axis=1, keepdims=True)).astype(np.float32)


def iota(shape, dim):
    return lax.broadcasted_iota(jnp.int32, shape, dim)


def near(*arrays):
    return [pltpu.with_memory_space_constraint(a, VMEM) for a in arrays]


def far_away(*arrays):
    return [pltpu.with_memory_space_constraint(a, pltpu.HBM) for a in arrays]


def two_halves(value):
    high = value.astype(BF16)
    return high, (value - high.astype(F32)).astype(BF16)


def dot(a, b, dims=((1,), (0,))):
    return lax.dot_general(a, b, (dims, ((), ())), preferred_element_type=F32)


def band(tap_of, weight):
    total = jnp.zeros(tap_of.shape, F32)
    for tap in range(TAPS):
        total = jnp.where(tap_of == tap, weight(tap), total)
    return two_halves(total)


def odd_block():
    return lax.rem(lax.axis_index("az"), 2) == 1


def in_order(partner, other):
    odd = odd_block()
    return [jnp.where(odd, partner, other), jnp.where(odd, other, partner)]


def swapped(to_partner, to_other):
    partner = lax.ppermute(to_partner, "az", [(0, 1), (1, 0), (2, 3), (3, 2)])
    other = lax.ppermute(to_other, "az", [(1, 2), (2, 1)])
    return partner, other


def resample_kernel(
    date,
    count,
    *refs,
):
    tables, (own, partner, other), rest = refs[:5], refs[5:8], refs[8:]
    stacks, power = rest[:count], rest[count]
    rows_in, edges, wide_hi, wide_lo, arrived, *local = rest[count + 1 :]
    loads = [
        pltpu.make_async_copy(table, here, arrived.at[4 + at])
        for at, (table, here) in enumerate(zip(tables, local))
    ]
    for load in loads:
        load.start()
    azs, rgs, azf, rgf, bank = local
    copies = [
        pltpu.make_async_copy(source.at[date], edges.at[at], arrived.at[2 + at])
        for at, source in enumerate((partner, other))
    ] + [
        pltpu.make_async_copy(own.at[date, part], rows_in.at[part, 0:ROWS], arrived.at[part])
        for part in range(2)
    ]
    for copy in copies:
        copy.start()
    for load in loads:
        load.wait()
    source = iota((ROWS, ROWS + 16), 1)
    source = jnp.where(
        source < ROWS, source, jnp.where(source < ROWS + 8, source - ROWS - 8, source - 8)
    )
    az_frac = azf[date]
    rg_frac = rgf[date]
    az_hi, az_lo = band(
        source - iota((ROWS, ROWS + 16), 0) - azs[date] + (TAPS // 2 - 1),
        lambda tap: bank[az_frac, tap],
    )
    az_both = jnp.concatenate([az_hi, az_lo], axis=0)
    half = TILE // 2
    rg_hi, rg_lo = band(
        iota((2 * TILE, TILE), 0) - half - iota((2 * TILE, TILE), 1) - rgs[date] + (TAPS // 2 - 1),
        lambda tap: bank[rg_frac, tap],
    )
    blank = jnp.zeros((ROWS, half), BF16)
    for part in range(2):
        if part == 0:
            copies[0].wait()
            copies[1].wait()
        pair = edges[0, part].astype(F32), edges[1, part].astype(F32)
        rows_in[part, ROWS : ROWS + 16] = jnp.concatenate(
            in_order(*pair), axis=0
        ).astype(BF16)
        copies[2 + part].wait()
        for tile in range(NT + 1):
            first = max(tile * TILE - half, 0)
            last = min(tile * TILE + half, COLS)
            both = dot(az_both, rows_in[part, :, first:last])
            pieces = two_halves(both[:ROWS] + both[ROWS:])
            for piece, wide in zip(pieces, (wide_hi, wide_lo)):
                if tile == 0:
                    piece = jnp.concatenate([blank, piece], axis=1)
                if tile == NT:
                    piece = jnp.concatenate([piece, blank], axis=1)
                place = part * ROWS
                if tile < NT:
                    at = tile * 2 * ROWS + place
                    wide[at : at + ROWS, 0:TILE] = piece
                if tile > 0:
                    at = (tile - 1) * 2 * ROWS + place
                    wide[at : at + ROWS, TILE : 2 * TILE] = piece
    at = 0
    for stack in stacks:
        size = stack.shape[0]
        hi, lo = wide_hi[at : at + size], wide_lo[at : at + size]
        stack[...] = dot(hi, rg_hi) + (dot(lo, rg_hi) + dot(hi, rg_lo))
        at += size
    power[...] = jnp.zeros(power.shape, F32)
    box = column_box()
    for tile in range(NT):
        s0, s1 = both_parts(stacks, tile)
        add_columns(power, box, tile, s0 * s0 + s1 * s1)


def column_box():
    reach = iota((32, TILE), 1) // LOOK_RG + 8 - iota((32, TILE), 0)
    return jnp.where(jnp.abs(reach) <= RADIUS, 1.0, 0.0).astype(BF16)


def both_parts(stacks, tile):
    at = tile * 2 * ROWS
    for stack in stacks:
        if at < stack.shape[0]:
            break
        at -= stack.shape[0]
    return stack[at : at + ROWS], stack[at + ROWS : at + 2 * ROWS]


def add_columns(columns, box, tile, values):
    high, low = two_halves(values)
    nt = ((1,), (1,))
    columns[tile * 16 : tile * 16 + 32] += dot(box, high, nt) + dot(box, low, nt)


def resample(date, far, scalars, slc, partner, other):
    spaces = (VMEM, pltpu.HBM) if far else (VMEM,)
    rows = NT * 2 * ROWS // len(spaces)
    return pl.pallas_call(
        functools.partial(resample_kernel, date, len(spaces)),
        compiler_params=GRANT,
        out_shape=tuple(space((rows, TILE), F32) for space in spaces)
        + (VMEM((LCOLS + 16, ROWS), F32),),
        in_specs=[pl.BlockSpec(memory_space=pl.ANY)] * 8,
        out_specs=(pl.BlockSpec(memory_space=VMEM),) * (len(spaces) + 1),
        scratch_shapes=[
            pltpu.VMEM((2, ROWS + 16, COLS), BF16),
            pltpu.VMEM((2, 2, 8, COLS), BF16),
            pltpu.VMEM((NT * 2 * ROWS, 2 * TILE), BF16),
            pltpu.VMEM((NT * 2 * ROWS, 2 * TILE), BF16),
            pltpu.SemaphoreType.DMA((9,)),
        ]
        + [SMEM((2,), jnp.int32)] * 4
        + [SMEM((KBANK, TAPS), F32)],
        cost_estimate=pl.CostEstimate(
            flops=3_000_000_000, transcendentals=0, bytes_accessed=1_600_000
        ),
    )(*far_away(*scalars, slc), partner, other)


FAR = NT * ROWS


def looks_kernel(center, near_first, second, power0, power1, far, out, columns, far_first, arrived):
    copy = pltpu.make_async_copy(far, far_first, arrived)
    copy.start()
    box = column_box()
    columns[...] = jnp.zeros(columns.shape, F32)
    for tile in range(NT):
        if tile == NT // 2:
            copy.wait()
        at = tile * TILE
        e0 = center[0:8, :, at : at + TILE].astype(F32).reshape(ROWS, TILE)
        e1 = center[8:16, :, at : at + TILE].astype(F32).reshape(ROWS, TILE)
        values = []
        for stacks in ((near_first, far_first), (second,)):
            s0, s1 = both_parts(stacks, tile)
            values += [e0 * s0 + e1 * s1, e1 * s0 - e0 * s1]
        values.append(e0 * e0 + e1 * e1)
        add_columns(columns, box, tile, jnp.concatenate(values, axis=0))

    total = jnp.zeros((LCOLS, 128), F32)
    quantity = 0
    for part in (columns, power0, power1):
        shape = (part.shape[1], 128)
        hit = iota(shape, 0) // LOOK_AZ == iota(shape, 1) - quantity * LOOKS
        box_rows = jnp.where(hit, 1.0 / (LOOK_AZ * LOOK_RG), 0.0).astype(BF16)
        high, low = two_halves(part[8 : 8 + LCOLS])
        total = total + (dot(high, box_rows) + dot(low, box_rows))
        quantity += part.shape[1] // ROWS
    out[...] = total


def looks(center, near_first, far_first, second, power0, power1):
    return pl.pallas_call(
        looks_kernel,
        name="looks",
        compiler_params=GRANT,
        out_shape=VMEM((LCOLS, 128), F32),
        in_specs=[pl.BlockSpec(memory_space=VMEM)] * 5 + [pl.BlockSpec(memory_space=pl.ANY)],
        out_specs=pl.BlockSpec(memory_space=VMEM),
        scratch_shapes=[
            pltpu.VMEM((LCOLS + 16, 5 * ROWS), F32),
            pltpu.VMEM((FAR, TILE), F32),
            pltpu.SemaphoreType.DMA,
        ],
    )(
        *near(center, near_first, second, power0, power1), *far_away(far_first)
    )


def coherence_kernel(own, partner, other, out, kept):
    source = iota((384, 384), 0)
    target = iota((384, 384), 1)
    row_in = source % 16 + (source // 128) * 16 - 16
    lane = source % 128
    quantity = lane // 16
    group = target // 128
    slot = target % 128
    date = slot // 32
    wanted = jnp.where(
        group == 0, date * 2 + slot % 2, jnp.where(group == 1, 5 + date, 4)
    )
    reach = row_in - (slot % 32) // 2
    hit = (quantity == wanted) & (jnp.abs(reach) <= RADIUS) & (slot < 64)
    box = jnp.where(hit, 1.0, 0.0).astype(BF16)
    before, after = in_order(partner[...], other[...])
    high, low = two_halves(jnp.concatenate([before, own[...], after], axis=1))
    summed = dot(high, box) + dot(low, box)
    cross = summed[:, 0:128]
    scale = 1.0 / jnp.sqrt(summed[:, 256:384] * summed[:, 128:256] + EPS)
    kept[...] = cross * scale
    third = LCOLS // 3
    pieces = [kept[pl.ds(k, third, stride=3), :] for k in range(3)]
    pair = jnp.concatenate([pieces[0][:, 0:64], pieces[1][:, 0:64]], axis=1)
    out[...] = jnp.stack([pair, pieces[2]], axis=1).astype(BF16)


def coherence(own, partner, other):
    return pl.pallas_call(
        coherence_kernel,
        name="coherence",
        compiler_params=GRANT,
        out_shape=VMEM((LCOLS // 3, 2, 128), BF16),
        in_specs=[pl.BlockSpec(memory_space=VMEM)] * 3,
        out_specs=pl.BlockSpec(memory_space=VMEM),
        scratch_shapes=[pltpu.VMEM((LCOLS, 128), F32)],
    )(*near(own, partner, other))


def finish_kernel(arrived, out, mean):
    source = iota((64, 128), 0)
    lane = iota((64, 128), 1)
    tn = ((0,), (0,))
    wide = arrived[...].astype(F32)
    packed = jnp.concatenate([wide[:, 0], wide[:, 1, 0:64]], axis=1).astype(BF16)
    placed = []
    for date in range(2):
        spread = jnp.where(lane == source * 2 + date, 1.0, 0.0).astype(BF16)
        placed.append(dot(packed, spread, tn))
    rows = jnp.concatenate(
        [placed[0][k * 64 : k * 64 + 32] + placed[1][k * 64 + 32 : k * 64 + 64] for k in range(3)],
        axis=0,
    )
    out[...] = rows.astype(BF16)
    square = rows * rows
    pair = jnp.where(iota((48, 96), 1) // 2 == iota((48, 96), 0), 1.0, 0.0)
    exact = lax.Precision.HIGHEST
    magnitude = jnp.sqrt(jnp.dot(pair, square, precision=exact, preferred_element_type=F32))
    share = jnp.full((8, 128), 1.0 / 128, F32)
    average = lax.dot_general(
        share, magnitude, (((1,), (1,)), ((), ())), precision=exact, preferred_element_type=F32
    )
    for k in range(3):
        mean[k : k + 1] = average[0:1, k * LOOKS : (k + 1) * LOOKS]


def finish(arrived):
    return pl.pallas_call(
        finish_kernel,
        name="finish",
        compiler_params=GRANT,
        out_shape=(
            jax.ShapeDtypeStruct((96, 128), BF16),
            jax.ShapeDtypeStruct((3, LOOKS), F32),
        ),
        in_specs=[pl.BlockSpec(memory_space=VMEM)],
        out_specs=(pl.BlockSpec(memory_space=VMEM), pl.BlockSpec(memory_space=VMEM)),
    )(*near(arrived))


def quarters_kernel(slc, *rest):
    *outs, to_partner, to_other, arrived = rest
    odd = odd_block()
    copies = []
    for out, start in (
        (to_partner, jnp.where(odd, 0, ROWS - 8)),
        (to_other, jnp.where(odd, ROWS - 8, 0)),
    ):
        source = slc.at[:, :, pl.ds(pl.multiple_of(start, 8), 8)]
        copies.append(pltpu.make_async_copy(source, out, arrived.at[len(copies)]))
    for out, *pair in zip(outs, *HOMES):
        for at, homes in enumerate(zip(*pair)):
            even_index, odd_index = [x * 4 + y for x, y in homes]
            index = jnp.where(odd, odd_index, even_index)
            part, block = lax.div(index, 8), lax.rem(index, 8)
            source = slc.at[0, part, pl.ds(pl.multiple_of(block * 8, 8), 8)]
            copies.append(pltpu.make_async_copy(source, out.at[at], arrived.at[len(copies)]))
    for copy in copies[2:] + copies[:2]:
        copy.start()
    for copy in copies:
        copy.wait()


def quarters_of(slc):
    return pl.pallas_call(
        quarters_kernel,
        name="quarters",
        compiler_params=GRANT,
        out_shape=(VMEM((4, 8, COLS), BF16),) * 4 + (VMEM((2, 2, 8, COLS), BF16),) * 2,
        in_specs=[pl.BlockSpec(memory_space=pl.ANY)],
        out_specs=(pl.BlockSpec(memory_space=VMEM),) * 6,
        scratch_shapes=[pltpu.SemaphoreType.DMA((18,))],
    )(*far_away(slc))


def copies_kernel(own, *rest):
    *pieces, out, value, sent = rest
    total = own[0]
    for piece in pieces:
        total = total + piece[0]
    value[...] = total
    copies = [pltpu.make_async_copy(value, out.at[at], sent.at[at]) for at in range(16)]
    for copy in copies:
        copy.start()
    for copy in copies:
        copy.wait()


def copies_of(own, pieces):
    return pl.pallas_call(
        copies_kernel,
        name="copies",
        compiler_params=GRANT,
        out_shape=pltpu.HBM((16, 8, COLS), BF16),
        in_specs=[pl.BlockSpec(memory_space=VMEM)] * 4,
        out_specs=pl.BlockSpec(memory_space=pl.ANY),
        scratch_shapes=[pltpu.VMEM((8, COLS), BF16), pltpu.SemaphoreType.DMA((16,))],
    )(*near(own, *pieces))


def place(z, x, y):
    return z * 16 + x * 4 + y


EVEN = (
    ((0, 0), (0, 3), (1, 3), (3, 3)),
    ((1, 0), (2, 0), (1, 1), (2, 1)),
    ((3, 0), (3, 1), (3, 2), (2, 3)),
    ((0, 1), (0, 2), (1, 2), (2, 2)),
)
HOMES = (EVEN, tuple(tuple((y, -x % 4) for x, y in homes) for homes in EVEN))


def send(value, hops):
    pairs = [
        (place(0, *source) * 4 + az, place(0, *target) * 4 + az)
        for az in range(4)
        for source, target in hops[az % 2]
    ]
    return lax.ppermute(value, ("date", "az"), pairs)


def body(slc, az_shift, rg_shift, az_frac, rg_frac):
    scalars = (az_shift, rg_shift, az_frac, rg_frac, jnp.asarray(kernel_bank()))
    *quarters, to_partner, to_other = quarters_of(slc)
    kept = jnp.where(lax.axis_index("date") == 0, quarters[0], jnp.zeros_like(quarters[0]))
    kept = lax.optimization_barrier(kept)

    pieces = [
        send(quarters[k], [[(homes[0][0], homes[k][0])] for homes in HOMES])
        for k in range(1, 4)
    ]
    edges = swapped(to_partner, to_other)
    quarter = kept + sum(pieces)

    pieces = [
        send(
            quarter[k : k + 1],
            [[(group[0], group[k]) for group in homes] for homes in HOMES],
        )
        for k in range(1, 4)
    ]
    chunk = quarter[0:1] + sum(pieces)

    flat = [home for group in EVEN for home in group]
    pieces = [
        lax.ppermute(chunk, "date", [(place(0, *home), place(k, *home)) for home in flat])
        for k in (1, 3, 2)
    ]
    first = resample(0, True, scalars, slc, *edges)
    pieces, first = lax.optimization_barrier((pieces, first))

    planes = [[place(z, x, y) for x in range(4) for y in range(4)] for z in range(4)]
    copies = copies_of(chunk, pieces)
    center = lax.all_to_all(copies, "date", 0, 0, axis_index_groups=planes, tiled=True)
    near_first, far_first, power0 = first
    second, power1 = resample(1, False, scalars, slc, *edges)
    own = looks(center, near_first, far_first, second, power0, power1)
    around = swapped(own, own)
    outgoing = coherence(own, *around)
    arrived = lax.all_to_all(outgoing, "date", split_axis=0, concat_axis=0, tiled=True)
    rows, mean = finish(arrived)
    return rows.reshape(3, LOOKS, 2, 128), mean


def solution(mesh):
    placed = (P("date", None, "az", None), P("date"), P("date"), P("date"), P("date"))
    return jax.shard_map(
        body,
        mesh=mesh,
        in_specs=placed,
        out_specs=(P("date", "az", None, None), P("date", "az")),
        check_vma=False,
    )
```

```python
import functools

import jax
import jax.numpy as jnp
import numpy as np
from jax import lax
from jax.experimental import pallas as pl
from jax.experimental.pallas import tpu as pltpu
from jax.sharding import PartitionSpec as P


TAPS = 8
KBANK = 16
LOOK_AZ = 4
LOOK_RG = 16
RADIUS = 3
EPS = 1e-06
ROWS = 64
COLS = 3072
TILE = 256
NT = COLS // TILE
LOOKS = ROWS // LOOK_AZ
LCOLS = COLS // LOOK_RG
F32 = jnp.float32
BF16 = jnp.bfloat16
VMEM = pltpu.VMEM
SMEM = pltpu.SMEM

GRANT = pltpu.CompilerParams(vmem_limit_bytes=20 * 2**20)


def kernel_bank():
    fraction = np.arange(KBANK)[:, None] / KBANK
    offset = np.arange(TAPS)[None, :] - (TAPS // 2 - 1) - fraction
    shaped = np.sinc(offset) * (0.5 + 0.5 * np.cos(np.pi * offset / (TAPS // 2 + 0.5)))
    return (shaped / shaped.sum(axis=1, keepdims=True)).astype(np.float32)


def iota(shape, dim):
    return lax.broadcasted_iota(jnp.int32, shape, dim)


def near(*arrays):
    return [pltpu.with_memory_space_constraint(a, VMEM) for a in arrays]


def far_away(*arrays):
    return [pltpu.with_memory_space_constraint(a, pltpu.HBM) for a in arrays]


def two_halves(value):
    high = value.astype(BF16)
    return high, (value - high.astype(F32)).astype(BF16)


def dot(a, b, dims=((1,), (0,))):
    return lax.dot_general(a, b, (dims, ((), ())), preferred_element_type=F32)


def band(tap_of, weight):
    total = jnp.zeros(tap_of.shape, F32)
    for tap in range(TAPS):
        total = jnp.where(tap_of == tap, weight(tap), total)
    return two_halves(total)


def odd_block():
    return lax.rem(lax.axis_index("az"), 2) == 1


def in_order(partner, other):
    odd = odd_block()
    return [jnp.where(odd, partner, other), jnp.where(odd, other, partner)]


def swapped(to_partner, to_other):
    partner = lax.ppermute(to_partner, "az", [(0, 1), (1, 0), (2, 3), (3, 2)])
    other = lax.ppermute(to_other, "az", [(1, 2), (2, 1)])
    return partner, other


def resample_kernel(
    date,
    count,
    *refs,
):
    tables, (own, partner, other), rest = refs[:5], refs[5:8], refs[8:]
    stacks, power = rest[:count], rest[count]
    rows_in, edges, wide_hi, wide_lo, arrived, *local = rest[count + 1 :]
    loads = [
        pltpu.make_async_copy(table, here, arrived.at[4 + at])
        for at, (table, here) in enumerate(zip(tables, local))
    ]
    for load in loads:
        load.start()
    azs, rgs, azf, rgf, bank, *held = local
    copies = [
        pltpu.make_async_copy(source.at[date], edges.at[at], arrived.at[2 + at])
        for at, source in enumerate((partner, other))
    ] + [
        pltpu.make_async_copy(own.at[date, part], rows_in.at[part, 0:ROWS], arrived.at[part])
        for part in range(2)
    ]
    for copy in copies:
        copy.start()
    for load in loads:
        load.wait()
    source = iota((ROWS, ROWS + 16), 1)
    source = jnp.where(
        source < ROWS, source, jnp.where(source < ROWS + 8, source - ROWS - 8, source - 8)
    )
    az_frac = azf[date]
    rg_frac = rgf[date]
    az_hi, az_lo = band(
        source - iota((ROWS, ROWS + 16), 0) - azs[date] + (TAPS // 2 - 1),
        lambda tap: bank[az_frac, tap],
    )
    az_both = jnp.concatenate([az_hi, az_lo], axis=0)
    half = TILE // 2
    rg_hi, rg_lo = band(
        iota((2 * TILE, TILE), 0) - half - iota((2 * TILE, TILE), 1) - rgs[date] + (TAPS // 2 - 1),
        lambda tap: bank[rg_frac, tap],
    )
    blank = jnp.zeros((ROWS, half), BF16)
    for part in range(2):
        if part == 0:
            copies[0].wait()
            copies[1].wait()
        pair = edges[0, part].astype(F32), edges[1, part].astype(F32)
        rows_in[part, ROWS : ROWS + 16] = jnp.concatenate(
            in_order(*pair), axis=0
        ).astype(BF16)
        copies[2 + part].wait()
        for tile in range(NT + 1):
            first = max(tile * TILE - half, 0)
            last = min(tile * TILE + half, COLS)
            both = dot(az_both, rows_in[part, :, first:last])
            pieces = two_halves(both[:ROWS] + both[ROWS:])
            for piece, wide in zip(pieces, (wide_hi, wide_lo)):
                if tile == 0:
                    piece = jnp.concatenate([blank, piece], axis=1)
                if tile == NT:
                    piece = jnp.concatenate([piece, blank], axis=1)
                place = part * ROWS
                if tile < NT:
                    at = tile * 2 * ROWS + place
                    wide[at : at + ROWS, 0:TILE] = piece
                if tile > 0:
                    at = (tile - 1) * 2 * ROWS + place
                    wide[at : at + ROWS, TILE : 2 * TILE] = piece
    far_copies = [
        pltpu.make_async_copy(here, out, arrived.at[9]) for here, out in zip(held, stacks[1:])
    ]
    stacks = [stacks[0], *held]
    size = stacks[0].shape[0]
    for half_of in reversed(range(count)):
        at = half_of * size
        hi, lo = wide_hi[at : at + size], wide_lo[at : at + size]
        stacks[half_of][...] = dot(hi, rg_hi) + (dot(lo, rg_hi) + dot(hi, rg_lo))
        if half_of:
            far_copies[0].start()
    power[...] = jnp.zeros(power.shape, F32)
    box = column_box()
    for tile in range(NT):
        s0, s1 = both_parts(stacks, tile)
        add_columns(power, box, tile, s0 * s0 + s1 * s1)
    for copy in far_copies:
        copy.wait()


def column_box():
    reach = iota((32, TILE), 1) // LOOK_RG + 8 - iota((32, TILE), 0)
    return jnp.where(jnp.abs(reach) <= RADIUS, 1.0, 0.0).astype(BF16)


def both_parts(stacks, tile):
    at = tile * 2 * ROWS
    for stack in stacks:
        if at < stack.shape[0]:
            break
        at -= stack.shape[0]
    return stack[at : at + ROWS], stack[at + ROWS : at + 2 * ROWS]


def add_columns(columns, box, tile, values):
    high, low = two_halves(values)
    nt = ((1,), (1,))
    columns[tile * 16 : tile * 16 + 32] += dot(box, high, nt) + dot(box, low, nt)


def resample(date, far, scalars, slc, partner, other):
    spaces = (VMEM, pltpu.HBM) if far else (VMEM,)
    rows = NT * 2 * ROWS // len(spaces)
    return pl.pallas_call(
        functools.partial(resample_kernel, date, len(spaces)),
        compiler_params=GRANT,
        out_shape=tuple(space((rows, TILE), F32) for space in spaces)
        + (VMEM((LCOLS + 16, ROWS), F32),),
        in_specs=[pl.BlockSpec(memory_space=pl.ANY)] * 8,
        out_specs=tuple(
            pl.BlockSpec(memory_space=VMEM if space is VMEM else pl.ANY) for space in spaces
        )
        + (pl.BlockSpec(memory_space=VMEM),),
        scratch_shapes=[
            pltpu.VMEM((2, ROWS + 16, COLS), BF16),
            pltpu.VMEM((2, 2, 8, COLS), BF16),
            pltpu.VMEM((NT * 2 * ROWS, 2 * TILE), BF16),
            pltpu.VMEM((NT * 2 * ROWS, 2 * TILE), BF16),
            pltpu.SemaphoreType.DMA((10,)),
        ]
        + [SMEM((2,), jnp.int32)] * 4
        + [SMEM((KBANK, TAPS), F32)]
        + [pltpu.VMEM((rows, TILE), F32)] * (len(spaces) - 1),
        cost_estimate=pl.CostEstimate(
            flops=3_000_000_000, transcendentals=0, bytes_accessed=1_600_000
        ),
    )(*far_away(*scalars, slc), partner, other)


FAR = NT * ROWS


def looks_kernel(center, near_first, second, power0, power1, far, out, columns, far_first, arrived):
    copy = pltpu.make_async_copy(far, far_first, arrived)
    copy.start()
    box = column_box()
    columns[...] = jnp.zeros(columns.shape, F32)
    for tile in range(NT):
        if tile == NT // 2:
            copy.wait()
        at = tile * TILE
        e0 = center[0:8, :, at : at + TILE].astype(F32).reshape(ROWS, TILE)
        e1 = center[8:16, :, at : at + TILE].astype(F32).reshape(ROWS, TILE)
        values = []
        for stacks in ((near_first, far_first), (second,)):
            s0, s1 = both_parts(stacks, tile)
            values += [e0 * s0 + e1 * s1, e1 * s0 - e0 * s1]
        values.append(e0 * e0 + e1 * e1)
        add_columns(columns, box, tile, jnp.concatenate(values, axis=0))

    total = jnp.zeros((LCOLS, 128), F32)
    quantity = 0
    for part in (columns, power0, power1):
        shape = (part.shape[1], 128)
        hit = iota(shape, 0) // LOOK_AZ == iota(shape, 1) - quantity * LOOKS
        box_rows = jnp.where(hit, 1.0 / (LOOK_AZ * LOOK_RG), 0.0).astype(BF16)
        high, low = two_halves(part[8 : 8 + LCOLS])
        total = total + (dot(high, box_rows) + dot(low, box_rows))
        quantity += part.shape[1] // ROWS
    out[...] = total


def looks(center, near_first, far_first, second, power0, power1):
    return pl.pallas_call(
        looks_kernel,
        name="looks",
        compiler_params=GRANT,
        out_shape=VMEM((LCOLS, 128), F32),
        in_specs=[pl.BlockSpec(memory_space=VMEM)] * 5 + [pl.BlockSpec(memory_space=pl.ANY)],
        out_specs=pl.BlockSpec(memory_space=VMEM),
        scratch_shapes=[
            pltpu.VMEM((LCOLS + 16, 5 * ROWS), F32),
            pltpu.VMEM((FAR, TILE), F32),
            pltpu.SemaphoreType.DMA,
        ],
    )(
        *near(center, near_first, second, power0, power1), *far_away(far_first)
    )


def coherence_kernel(own, partner, other, out, kept):
    source = iota((384, 384), 0)
    target = iota((384, 384), 1)
    row_in = source % 16 + (source // 128) * 16 - 16
    lane = source % 128
    quantity = lane // 16
    group = target // 128
    slot = target % 128
    date = slot // 32
    wanted = jnp.where(
        group == 0, date * 2 + slot % 2, jnp.where(group == 1, 5 + date, 4)
    )
    reach = row_in - (slot % 32) // 2
    hit = (quantity == wanted) & (jnp.abs(reach) <= RADIUS) & (slot < 64)
    box = jnp.where(hit, 1.0, 0.0).astype(BF16)
    before, after = in_order(partner[...], other[...])
    high, low = two_halves(jnp.concatenate([before, own[...], after], axis=1))
    summed = dot(high, box) + dot(low, box)
    cross = summed[:, 0:128]
    scale = 1.0 / jnp.sqrt(summed[:, 256:384] * summed[:, 128:256] + EPS)
    kept[...] = cross * scale
    third = LCOLS // 3
    pieces = [kept[pl.ds(k, third, stride=3), :] for k in range(3)]
    pair = jnp.concatenate([pieces[0][:, 0:64], pieces[1][:, 0:64]], axis=1)
    out[...] = jnp.stack([pair, pieces[2]], axis=1).astype(BF16)


def coherence(own, partner, other):
    return pl.pallas_call(
        coherence_kernel,
        name="coherence",
        compiler_params=GRANT,
        out_shape=VMEM((LCOLS // 3, 2, 128), BF16),
        in_specs=[pl.BlockSpec(memory_space=VMEM)] * 3,
        out_specs=pl.BlockSpec(memory_space=VMEM),
        scratch_shapes=[pltpu.VMEM((LCOLS, 128), F32)],
    )(*near(own, partner, other))


def finish_kernel(arrived, out, mean):
    source = iota((64, 128), 0)
    lane = iota((64, 128), 1)
    tn = ((0,), (0,))
    wide = arrived[...].astype(F32)
    packed = jnp.concatenate([wide[:, 0], wide[:, 1, 0:64]], axis=1).astype(BF16)
    placed = []
    for date in range(2):
        spread = jnp.where(lane == source * 2 + date, 1.0, 0.0).astype(BF16)
        placed.append(dot(packed, spread, tn))
    rows = jnp.concatenate(
        [placed[0][k * 64 : k * 64 + 32] + placed[1][k * 64 + 32 : k * 64 + 64] for k in range(3)],
        axis=0,
    )
    out[...] = rows.astype(BF16)
    square = rows * rows
    pair = jnp.where(iota((48, 96), 1) // 2 == iota((48, 96), 0), 1.0, 0.0)
    exact = lax.Precision.HIGHEST
    magnitude = jnp.sqrt(jnp.dot(pair, square, precision=exact, preferred_element_type=F32))
    share = jnp.full((8, 128), 1.0 / 128, F32)
    average = lax.dot_general(
        share, magnitude, (((1,), (1,)), ((), ())), precision=exact, preferred_element_type=F32
    )
    for k in range(3):
        mean[k : k + 1] = average[0:1, k * LOOKS : (k + 1) * LOOKS]


def finish(arrived):
    return pl.pallas_call(
        finish_kernel,
        name="finish",
        compiler_params=GRANT,
        out_shape=(
            jax.ShapeDtypeStruct((96, 128), BF16),
            jax.ShapeDtypeStruct((3, LOOKS), F32),
        ),
        in_specs=[pl.BlockSpec(memory_space=VMEM)],
        out_specs=(pl.BlockSpec(memory_space=VMEM), pl.BlockSpec(memory_space=VMEM)),
    )(*near(arrived))


def quarters_kernel(slc, *rest):
    *outs, to_partner, to_other, arrived = rest
    odd = odd_block()
    copies = []
    for out, start in (
        (to_partner, jnp.where(odd, 0, ROWS - 8)),
        (to_other, jnp.where(odd, ROWS - 8, 0)),
    ):
        source = slc.at[:, :, pl.ds(pl.multiple_of(start, 8), 8)]
        copies.append(pltpu.make_async_copy(source, out, arrived.at[len(copies)]))
    for out, *pair in zip(outs, *HOMES):
        for at, homes in enumerate(zip(*pair)):
            even_index, odd_index = [x * 4 + y for x, y in homes]
            index = jnp.where(odd, odd_index, even_index)
            part, block = lax.div(index, 8), lax.rem(index, 8)
            source = slc.at[0, part, pl.ds(pl.multiple_of(block * 8, 8), 8)]
            copies.append(pltpu.make_async_copy(source, out.at[at], arrived.at[len(copies)]))
    for copy in copies[2:] + copies[:2]:
        copy.start()
    for copy in copies:
        copy.wait()


def quarters_of(slc):
    return pl.pallas_call(
        quarters_kernel,
        name="quarters",
        compiler_params=GRANT,
        out_shape=(VMEM((4, 8, COLS), BF16),) * 4 + (VMEM((2, 2, 8, COLS), BF16),) * 2,
        in_specs=[pl.BlockSpec(memory_space=pl.ANY)],
        out_specs=(pl.BlockSpec(memory_space=VMEM),) * 6,
        scratch_shapes=[pltpu.SemaphoreType.DMA((18,))],
    )(*far_away(slc))


def copies_kernel(own, *rest):
    *pieces, out, value, sent = rest
    total = own[0]
    for piece in pieces:
        total = total + piece[0]
    value[...] = total
    copies = [pltpu.make_async_copy(value, out.at[at], sent.at[at]) for at in range(16)]
    for copy in copies:
        copy.start()
    for copy in copies:
        copy.wait()


def copies_of(own, pieces):
    return pl.pallas_call(
        copies_kernel,
        name="copies",
        compiler_params=GRANT,
        out_shape=pltpu.HBM((16, 8, COLS), BF16),
        in_specs=[pl.BlockSpec(memory_space=VMEM)] * 4,
        out_specs=pl.BlockSpec(memory_space=pl.ANY),
        scratch_shapes=[pltpu.VMEM((8, COLS), BF16), pltpu.SemaphoreType.DMA((16,))],
    )(*near(own, *pieces))


def place(z, x, y):
    return z * 16 + x * 4 + y


EVEN = (
    ((0, 0), (0, 3), (1, 3), (3, 3)),
    ((1, 0), (2, 0), (1, 1), (2, 1)),
    ((3, 0), (3, 1), (3, 2), (2, 3)),
    ((0, 1), (0, 2), (1, 2), (2, 2)),
)
HOMES = (EVEN, tuple(tuple((y, -x % 4) for x, y in homes) for homes in EVEN))


def send(value, hops):
    pairs = [
        (place(0, *source) * 4 + az, place(0, *target) * 4 + az)
        for az in range(4)
        for source, target in hops[az % 2]
    ]
    return lax.ppermute(value, ("date", "az"), pairs)


def body(slc, az_shift, rg_shift, az_frac, rg_frac):
    scalars = (az_shift, rg_shift, az_frac, rg_frac, jnp.asarray(kernel_bank()))
    *quarters, to_partner, to_other = quarters_of(slc)
    kept = jnp.where(lax.axis_index("date") == 0, quarters[0], jnp.zeros_like(quarters[0]))
    kept = lax.optimization_barrier(kept)

    pieces = [
        send(quarters[k], [[(homes[0][0], homes[k][0])] for homes in HOMES])
        for k in range(1, 4)
    ]
    edges = swapped(to_partner, to_other)
    quarter = kept + sum(pieces)

    pieces = [
        send(
            quarter[k : k + 1],
            [[(group[0], group[k]) for group in homes] for homes in HOMES],
        )
        for k in range(1, 4)
    ]
    chunk = quarter[0:1] + sum(pieces)

    flat = [home for group in EVEN for home in group]
    pieces = [
        lax.ppermute(chunk, "date", [(place(0, *home), place(k, *home)) for home in flat])
        for k in (1, 3, 2)
    ]
    first = resample(0, True, scalars, slc, *edges)
    pieces, first = lax.optimization_barrier((pieces, first))

    planes = [[place(z, x, y) for x in range(4) for y in range(4)] for z in range(4)]
    copies = copies_of(chunk, pieces)
    center = lax.all_to_all(copies, "date", 0, 0, axis_index_groups=planes, tiled=True)
    near_first, far_first, power0 = first
    second, power1 = resample(1, False, scalars, slc, *edges)
    own = looks(center, near_first, far_first, second, power0, power1)
    around = swapped(own, own)
    outgoing = coherence(own, *around)
    arrived = lax.all_to_all(outgoing, "date", split_axis=0, concat_axis=0, tiled=True)
    rows, mean = finish(arrived)
    return rows.reshape(3, LOOKS, 2, 128), mean


def solution(mesh):
    placed = (P("date", None, "az", None), P("date"), P("date"), P("date"), P("date"))
    return jax.shard_map(
        body,
        mesh=mesh,
        in_specs=placed,
        out_specs=(P("date", "az", None, None), P("date", "az")),
        check_vma=False,
    )
```
